32 devices in a mesh: cp: 4 (over z), tp: 8 (over y, x, core).
Axes of the slice: x: 2, y: 2, z: 4, core: 2. Of those that a mesh axis runs over, the one named last changes fastest.
Arguments:
- checkpoint: bfloat16 [2048, 8192], P('cp', 'tp'), may hold values from -6 to 6
- norm_gain: float32 [8192], replicated, may hold values from 0.1 to 1.9
- query_weight: bfloat16 [8192, 8192], P(None, 'tp'), may hold values from -4 to 4
- key_weight: bfloat16 [8192, 1024], P(None, 'tp'), may hold values from -1 to 1
- value_weight: bfloat16 [8192, 1024], P(None, 'tp'), may hold values from -0.0625 to 0.0625
- output_weight: bfloat16 [8192, 8192], P('tp'), may hold values from -0.09375 to 0.09375
- block_order: int32 [8], replicated, may hold values from 0 to 7, each once
Outputs:
- projected: bfloat16 [2048, 8192], P('cp', 'tp')
- log_normalizer: float32 [64, 2048], P('tp', 'cp')
The draws below stay inside these ranges and needn't reach their ends.
Inputs may be any that keep to these rules, and one draw needn't show every extreme that they name: `block_order`: each of 0 to 7 once.
All inputs are finite; a program needn't handle non-finite values.
Results may differ from the reference program's by a relative error of at most 0.019.
Values may be sent and summed in bfloat16 or wider, within the bound.
A program may use at most 128 MiB of HBM per device.

```python
import math
import jax
import jax.numpy as jnp
from jax import lax

D = 8192
HEADS = 64
KV_HEADS = 8
HEAD_DIM = 128
SEQ = 2048
BLOCK = 256
N_CP = 4
N_TP = 8


def joint_query_key(key):
    shared_keys = jax.random.normal(jax.random.fold_in(key, 17), (D, KV_HEADS * HEAD_DIM), jnp.float32) / math.sqrt(D)
    shared_keys = jnp.clip(shared_keys, -1.0, 1.0)
    queries = jax.random.normal(jax.random.fold_in(key, 29), (D, HEADS * HEAD_DIM), jnp.float32) * (2.5 / math.sqrt(D))
    queries = jnp.clip(queries, -4.0, 4.0)
    return (queries, shared_keys)


def draw_query_weight(key, part):
    return joint_query_key(key)[0].astype(jnp.bfloat16)


def draw_key_weight(key, part):
    return joint_query_key(key)[1].astype(jnp.bfloat16)


def raised(values, stream_key, source, target, parts, factor):
    def block_of(axis_at):
        return (jnp.arange(values.shape[axis_at]) // (values.shape[axis_at] // parts)).reshape((-1,) + (1,) * (values.ndim - 1 - axis_at))

    first = jax.random.permutation(stream_key, parts)[block_of(target)]
    second = (block_of(target) + parts // 2) % parts
    return jnp.where((block_of(source) == first) | (block_of(source) == second), factor * values, values)


def steps_of(rng, dims, cuts, smallest, largest):
    def one(dim, blocks):
        steps = jax.random.uniform(jax.random.fold_in(jax.random.fold_in(rng, 6), dim), (blocks,), jnp.float32, smallest / len(cuts), largest / len(cuts))
        return jnp.repeat(jnp.exp(steps), dims[dim] // blocks).reshape((-1,) + (1,) * (len(dims) - dim - 1))

    gain = one(*cuts[0])
    for cut in cuts[1:]:
        gain = gain * one(*cut)
    return gain


def scatter_about(own_key, dims, spread, limit, shards=(), held_as=jnp.bfloat16):
    result = spread * jax.random.normal(own_key, dims, jnp.float32)
    if shards:
        result = result * steps_of(own_key, dims, shards, -0.22, 0.18)
    return jnp.clip(result, -limit, limit).astype(held_as)


def heavy_noise(own_key, shape, spread, limit, cuts, heavy, kind=jnp.bfloat16):
    entries = spread * jax.random.normal(own_key, shape, jnp.float32)
    if cuts:
        entries = entries * steps_of(own_key, shape, cuts, -0.22, 0.18)
    return jnp.clip(raised(entries, jax.random.fold_in(own_key, 3), *heavy), -limit, limit).astype(kind)


def setup_inputs(seed: int = 0) -> dict:
    streams_of = jax.random.split(jax.random.key(seed), 8)
    checkpoint = scatter_about(streams_of[0], (SEQ, D), 1.0, 6.0, ((0, 4), (1, 8)))
    norm_gain = jnp.clip(1.0 + 0.18 * jax.random.normal(streams_of[1], (D,), jnp.float32), 0.1, 1.9)
    query_weight = draw_query_weight(jax.random.fold_in(streams_of[7], 71), 0)
    key_weight = draw_key_weight(jax.random.fold_in(streams_of[7], 71), 0)
    value_weight = scatter_about(streams_of[4], (D, KV_HEADS * HEAD_DIM), D ** -0.5, 0.0625, ((1, 8),))
    output_weight = heavy_noise(streams_of[5], (HEADS * HEAD_DIM, D), (HEADS * HEAD_DIM) ** -0.5, 0.09375, ((0, 8),), (0, 1, 8, 2.0))
    block_order = jax.random.permutation(streams_of[6], 2 * N_CP).astype(jnp.int32)
    return {"checkpoint": checkpoint, "norm_gain": norm_gain, "query_weight": query_weight, "key_weight": key_weight, "value_weight": value_weight, "output_weight": output_weight, "block_order": block_order}


rope_base = 500000.0
norm_epsilon = 1e-05

def turn_pairs(matrix, positions, first_pair):
    pair_count = matrix.shape[-1] // 2
    pair_index = (first_pair + jnp.arange(pair_count, dtype=jnp.int32)).astype(jnp.float32)
    inverse_rates = rope_base ** (-2.0 * pair_index / HEAD_DIM)
    angles = positions.astype(jnp.float32)[:, None] * inverse_rates[None, :]
    cosine = jnp.cos(angles)[:, None, :]
    sine_part = jnp.sin(angles)[:, None, :]
    paired = matrix.reshape(matrix.shape[0], matrix.shape[1], pair_count, 2)
    former = paired[..., 0]
    latter = paired[..., 1]
    turned = jnp.stack([former * cosine - latter * sine_part, former * sine_part + latter * cosine], axis=-1)
    return turned.reshape(matrix.shape)

def reference(checkpoint, norm_gain, query_weight, key_weight, value_weight, output_weight, block_order):
    seq_rows = jnp.arange(SEQ, dtype=jnp.int32)
    positions = (block_order[seq_rows // BLOCK] * BLOCK + seq_rows % BLOCK).astype(jnp.int32)
    widened = checkpoint.astype(jnp.float32)
    mean_square = lax.optimization_barrier(jnp.mean(widened * widened, axis=-1, keepdims=True))
    normed = (widened * lax.rsqrt(mean_square + norm_epsilon) * norm_gain).astype(jnp.bfloat16)
    query_features = jnp.dot(normed, query_weight, preferred_element_type=jnp.float32)
    key_features = jnp.dot(normed, key_weight, preferred_element_type=jnp.float32)
    value_features = jnp.dot(normed, value_weight, preferred_element_type=jnp.float32)
    queries = turn_pairs(query_features.reshape(SEQ, HEADS, HEAD_DIM), positions, 0).astype(jnp.bfloat16)
    keys = turn_pairs(key_features.reshape(SEQ, KV_HEADS, HEAD_DIM), positions, 0).astype(jnp.bfloat16)
    values = value_features.astype(jnp.bfloat16).reshape(SEQ, KV_HEADS, HEAD_DIM)
    by_head_queries = jnp.transpose(queries, (1, 0, 2))
    key_heads = jnp.transpose(keys, (1, 0, 2))
    value_heads = jnp.transpose(values, (1, 0, 2))
    group_size = HEADS // KV_HEADS
    allowed = positions[None, :] <= positions[:, None]
    score_scale = 1.0 / math.sqrt(HEAD_DIM)

    def one_head(head_index):
        query_block = lax.dynamic_index_in_dim(by_head_queries, head_index, 0, keepdims=False)
        key_block = lax.dynamic_index_in_dim(key_heads, head_index // group_size, 0, keepdims=False)
        value_block = lax.dynamic_index_in_dim(value_heads, head_index // group_size, 0, keepdims=False)
        scores = jnp.dot(query_block, key_block.T, preferred_element_type=jnp.float32) * score_scale
        scores = jnp.where(allowed, scores, -jnp.inf)
        row_top = lax.optimization_barrier(jnp.max(scores, axis=-1, keepdims=True))
        normalizer = row_top + jnp.log(lax.optimization_barrier(jnp.sum(jnp.exp(scores - row_top), axis=-1, keepdims=True)))
        weights = jnp.exp(scores - normalizer).astype(jnp.bfloat16)
        attended_head = jnp.dot(weights, value_block, preferred_element_type=jnp.float32).astype(jnp.bfloat16)
        return (attended_head, normalizer[:, 0])
    attended, log_normalizer = lax.map(one_head, jnp.arange(HEADS, dtype=jnp.int32))
    attended_flat = jnp.transpose(attended, (1, 0, 2)).reshape(SEQ, HEADS * HEAD_DIM)
    group_rows = HEADS * HEAD_DIM // N_TP
    attended_groups = jnp.transpose(attended_flat.reshape(SEQ, N_TP, group_rows), (1, 0, 2))
    weight_groups = output_weight.reshape(N_TP, group_rows, D)

    def add_group(running_total, pieces):
        group_term = jnp.dot(pieces[0], pieces[1], preferred_element_type=jnp.float32).astype(jnp.bfloat16)
        group_term = lax.optimization_barrier(group_term)
        return (running_total + group_term.astype(jnp.float32), None)
    running_total, unused = lax.scan(add_group, jnp.zeros((SEQ, D), jnp.float32), (attended_groups, weight_groups))
    return (running_total.astype(jnp.bfloat16), log_normalizer)
```

```python
import functools
import math

import jax
import jax.numpy as jnp
import numpy as np
from jax import lax
from jax.experimental import pallas as pl
from jax.experimental.pallas import tpu as pltpu
from jax.sharding import PartitionSpec as P

HEAD_DIM = 128
KV_HEADS = 8
MESH = pl.DeviceIdType.MESH
VMEM_BYTES = 62 * 1024 * 1024
FUSED_BYTES = 67_000_000

rope_base = 500000.0
norm_epsilon = 1e-05
masked_score = -1e30
LOG2E = 1.4426950408889634


def partner_2(block, axis, stride):
    count = lax.axis_size(axis)
    route = []
    for low in range(count):
        high = low | 1 << stride
        if high != low and high < count:
            route += [(low, high), (high, low)]
    return lax.ppermute(block, axis, route)


def turn_pairs(matrix, positions, first_pair):
    pair_count = matrix.shape[-1] // 2
    pair_index = (first_pair + jnp.arange(pair_count, dtype=jnp.int32)).astype(jnp.float32)
    inverse_rates = rope_base ** (-2.0 * pair_index / HEAD_DIM)
    angles = positions.astype(jnp.float32)[:, None] * inverse_rates[None, :]
    cosine = jnp.cos(angles)[:, None, :]
    sine_part = jnp.sin(angles)[:, None, :]
    paired = matrix.reshape(matrix.shape[0], matrix.shape[1], pair_count, 2)
    former = paired[..., 0]
    latter = paired[..., 1]
    turned = jnp.stack(
        [former * cosine - latter * sine_part, former * sine_part + latter * cosine], axis=-1
    )
    return turned.reshape(matrix.shape)


def project_any(checkpoint, norm_gain, query_weight, key_weight, value_weight, positions):
    rows = checkpoint.shape[0]
    heads = query_weight.shape[1] // HEAD_DIM
    key_columns = key_weight.shape[1]
    gathered = lax.all_gather(checkpoint, "tp", axis=1, tiled=True)
    widened = gathered.astype(jnp.float32)
    mean_square = jnp.mean(widened * widened, axis=-1, keepdims=True)
    normed = (widened * lax.rsqrt(mean_square + norm_epsilon) * norm_gain).astype(jnp.bfloat16)
    query_features = jnp.dot(normed, query_weight, preferred_element_type=jnp.float32)
    key_features = jnp.dot(normed, key_weight, preferred_element_type=jnp.float32)
    value_features = jnp.dot(normed, value_weight, preferred_element_type=jnp.float32)
    turned = turn_pairs(query_features.reshape(rows, heads, HEAD_DIM), positions, 0)
    queries = (turned * (LOG2E / math.sqrt(HEAD_DIM))).astype(jnp.bfloat16)
    sharing = lax.axis_size("tp") // KV_HEADS
    part_of_head = lax.axis_index("tp") % sharing
    key_part = turn_pairs(
        key_features.reshape(rows, 1, key_columns), positions, part_of_head * (key_columns // 2)
    )
    key_part = key_part.astype(jnp.bfloat16).reshape(rows, key_columns)
    own_pair = jnp.stack([key_part, value_features.astype(jnp.bfloat16)])
    key_value = own_pair
    if sharing == 2:
        partner = partner_2(own_pair, "tp", 0)
        lower_first = jnp.concatenate([own_pair, partner], axis=-1)
        upper_first = jnp.concatenate([partner, own_pair], axis=-1)
        key_value = jnp.where(part_of_head == 0, lower_first, upper_first)
    return (
        queries.reshape(rows, heads * HEAD_DIM),
        jnp.concatenate([key_value[0], key_value[1]], axis=-1),
    )


def flipped(me, offset):
    result = me
    for bit in (1, 2, 4):
        chosen = offset // bit % 2
        result = result + chosen * (bit - 2 * bit * (me // bit % 2))
    return result


def greet(axis, others):
    barrier = pltpu.get_barrier_semaphore()
    for other in others:
        pl.semaphore_signal(barrier, inc=1, device_id={axis: other}, device_id_type=MESH)
    pl.semaphore_wait(barrier, len(others))


def attend_kernel(
    n_cp, order_ref, q_ref, kv_hbm, out_ref, norm_ref,
    ring, extended, bias, top, weighted, norms, kv_sem, send_sems, recv_sems,
):
    me = lax.axis_index("cp")
    rows = q_ref.shape[0]
    block = rows // 2
    heads = q_ref.shape[1] // HEAD_DIM
    right, left = lax.rem(me + 1, n_cp), lax.rem(me + n_cp - 1, n_cp)
    own_copy = pltpu.make_async_copy(kv_hbm, ring.at[0], kv_sem)
    own_copy.start()
    greet("cp", (right, left))
    own_copy.wait()

    def hop(step, h):
        at = pl.ds(h * block, block)
        return pltpu.make_async_remote_copy(
            src_ref=ring.at[step, at, :],
            dst_ref=ring.at[step + 1, at, :],
            send_sem=send_sems.at[step, h],
            recv_sem=recv_sems.at[step, h],
            device_id={"cp": right},
            device_id_type=MESH,
        )

    hop(0, 0).start()
    hop(0, 1).start()
    extended[:, HEAD_DIM:] = jnp.ones((rows, HEAD_DIM), jnp.bfloat16)
    top[...] = jnp.full(top.shape, masked_score, jnp.float32)
    weighted[...] = jnp.zeros_like(weighted)

    def visit(step, carried):
        for h in range(2):

            @pl.when(step > 0)
            def _():
                hop(step - 1, h).wait_recv()

            @pl.when(jnp.logical_and(step > 0, step < n_cp - 1))
            def _():
                hop(step, h).start()

        owner = lax.rem(me - step + n_cp, n_cp)
        extended[:, :HEAD_DIM] = ring[step, :, HEAD_DIM:]
        base = lax.broadcasted_iota(jnp.int32, (block, block), 0) - lax.broadcasted_iota(
            jnp.int32, (block, block), 1
        )
        for i in range(2):
            for j in range(2):
                ahead = (order_ref[2 * me + i] - order_ref[2 * owner + j]) * block
                bias[i * block : (i + 1) * block, j * block : (j + 1) * block] = jnp.where(
                    base + ahead >= 0, 0.0, masked_score
                )

        def one_head(h, inner):
            cols = pl.ds(pl.multiple_of(h * HEAD_DIM, HEAD_DIM), HEAD_DIM)
            keys = ring[step, :, :HEAD_DIM]
            for i in range(2):
                at = pl.ds(i * block, block)
                scores = lax.dot_general(
                    q_ref[at, cols], keys, (((1,), (1,)), ((), ())),
                    preferred_element_type=jnp.float32,
                )
                scores = scores + bias[at, :]
                old_top = top[h, at, :]
                new_top = jnp.maximum(old_top, jnp.max(scores, axis=1, keepdims=True))
                weights = jnp.exp2(scores - new_top).astype(jnp.bfloat16)
                shrink = jnp.exp2(old_top - new_top)
                top[h, at, :] = new_top
                weighted[h, at, :] = weighted[h, at, :] * shrink + jnp.dot(
                    weights, extended[...], preferred_element_type=jnp.float32
                )
            return inner

        lax.fori_loop(0, heads, one_head, 0, unroll=2)
        return carried

    lax.fori_loop(0, n_cp, visit, 0)
    lane = lax.broadcasted_iota(jnp.int32, (rows, HEAD_DIM), 1)
    norms[...] = jnp.zeros_like(norms)
    for h in range(heads):
        totals = weighted[h, :, HEAD_DIM:]
        out_ref[:, h * HEAD_DIM : (h + 1) * HEAD_DIM] = (
            weighted[h, :, :HEAD_DIM] / totals
        ).astype(jnp.bfloat16)
        norm = (top[h] + jnp.log2(totals)) * (1.0 / LOG2E)
        norms[...] = jnp.where(lane == h, norm, norms[...])
    norm_ref[...] = jnp.transpose(norms[...])[:heads, :]

    for step in range(n_cp - 1):
        for h in range(2):
            hop(step, h).wait_send()


def layer_kernel(
    order_ref, x_hbm, gain_hbm, wq_hbm, wk_hbm, wv_hbm, wo_hbm, turns_hbm, starts_hbm,
    out_ref, norm_ref,
    held, weights, out_weights, gains, acc, scaled, squares, turns, starts,
    queries, keys, values, weighted, top, attended, from_sib, from_six, from_x, from_y,
    x_sems, w_sems, o_sems, t_sems, ag_send, ag_recv, kv_send, kv_recv, rs_send, rs_recv,
):
    me = lax.axis_index("tp")
    z = lax.axis_index("cp")
    rows, depth = x_hbm.shape
    half = depth // 2
    block = rows // 2
    q_cols = wq_hbm.shape[1]
    k_cols = wk_hbm.shape[1]
    heads = q_cols // HEAD_DIM
    kv_end = q_cols + 2 * k_cols
    sib, nx, ny = flipped(me, 1), flipped(me, 2), flipped(me, 4)
    pieces = ((0, block), (block, block // 2), (block + block // 2, block // 2))

    upper = z // 2
    low = z + upper * (3 - 2 * z)
    others = []
    for k in range(3):
        near = k + 1 - (low if k == 0 else 0)
        others.append(near + upper * (3 - 2 * near))

    def ring(k):
        near = k + 1 - low * ((3 - k) // 3)
        return near + upper * (3 - 2 * near)

    x_copies = []
    for p, (first, count) in enumerate(((0, block), (block, block))):
        for h in range(2):
            at = pl.ds(first, count)
            x_copies.append(
                pltpu.make_async_copy(
                    x_hbm.at[at, pl.ds(h * half, half)], held.at[0, h, at, :], x_sems.at[p, h]
                )
            )
    for copy in x_copies:
        copy.start()
    small = [
        pltpu.make_async_copy(gain_hbm, gains, t_sems.at[0]),
        pltpu.make_async_copy(turns_hbm, turns, t_sems.at[1]),
        pltpu.make_async_copy(starts_hbm, starts, t_sems.at[2]),
    ]
    small[0].start()
    w_copies = []
    for e in range(8):
        chunk = pl.ds(pl.multiple_of(flipped(me, e) * depth, depth), depth)
        parts = ((wq_hbm, 0, q_cols), (wk_hbm, q_cols, k_cols), (wv_hbm, q_cols + k_cols, k_cols))
        w_copies.append(
            [
                pltpu.make_async_copy(
                    w.at[chunk, :], weights.at[e, :, pl.ds(at, size)], w_sems.at[e, i]
                )
                for i, (w, at, size) in enumerate(parts)
            ]
        )
    for copies in w_copies:
        for copy in copies:
            copy.start()
    small[1].start()
    small[2].start()
    o_copies = {}
    for e in (7, 6, 3, 2, 5, 4, 1, 0):
        for h in range(2):
            at = pl.ds(pl.multiple_of(flipped(me, e) * depth + h * half, half), half)
            o_copies[e, h] = pltpu.make_async_copy(
                wo_hbm.at[:, at], out_weights.at[e, h], o_sems.at[e, h]
            )

    barrier = pltpu.get_barrier_semaphore()
    peers = [{"tp": sib}, {"tp": nx}, {"tp": ny}] + [{"cp": other} for other in others]
    for peer in peers:
        pl.semaphore_signal(barrier, inc=1, device_id=peer, device_id_type=MESH)
    pl.semaphore_wait(barrier, len(peers))

    def remote(source, target, send, recv, device):
        return pltpu.make_async_remote_copy(
            src_ref=source, dst_ref=target, send_sem=send, recv_sem=recv,
            device_id=device, device_id_type=MESH,
        )

    gather = []
    for p, (first, count) in enumerate(pieces):
        at = pl.ds(first, count)

        def part(slot, h, at=at):
            return held.at[slot, h, at, :]

        plan = {
            "dx0": (0, 0, 2, nx), "dx1": (0, 1, 2, nx), "dy0": (0, 0, 4, ny), "dy1": (0, 1, 4, ny),
            "s0": (0, 0, 1, sib), "s1": (0, 1, 1, sib), "fy": (2, 0, 6, ny), "fx": (4, 1, 6, nx),
            "a0": (2, 0, 3, sib), "a1": (2, 1, 3, sib), "b0": (4, 0, 5, sib), "b1": (4, 1, 5, sib),
            "c0": (6, 0, 7, sib), "c1": (6, 1, 7, sib),
        }
        gather.append(
            {
                name: remote(
                    part(slot, h), part(to, h), ag_send.at[p, i], ag_recv.at[p, i], {"tp": other}
                )
                for i, (name, (slot, h, to, other)) in enumerate(plan.items())
            }
        )

    def send(p, *names):
        for name in names:
            gather[p][name].start()

    def landed(p, *names):
        for name in names:
            gather[p][name].wait_recv()

    for copy in x_copies[:2]:
        copy.wait()
    send(0, "dx0", "dy1", "dx1", "dy0", "s0", "s1")
    acc[...] = jnp.zeros_like(acc)
    squares[...] = jnp.zeros_like(squares)
    values[:, HEAD_DIM:, :] = jnp.ones((4, 16, rows), jnp.bfloat16)
    for copy in x_copies[2:]:
        copy.wait()
    for p in (1, 2):
        send(p, "s0", "s1")
    small[0].wait()

    def weights_of(*slots):
        for e in slots:
            for copy in w_copies[e]:
                copy.wait()

    def process(first, count, chunks, chunk_of):
        @pl.loop(0, chunks)
        def _(i):
            e, h = chunk_of(i)
            source = flipped(me, e)

            @pl.loop(0, count // 64)
            def _(j):
                at = pl.ds(pl.multiple_of(first + j * 64, 64), 64)
                into = pl.ds(pl.multiple_of(j * 64, 64), 64)
                wide = held[e, h, at, :].astype(jnp.float32)
                squares[at, :] += jnp.sum(wide * wide, axis=1, keepdims=True)
                scaled[into, :] = (wide * gains[source, h]).astype(jnp.bfloat16)

            acc[first : first + count, :] += jnp.dot(
                scaled[:count, :],
                weights[e, pl.ds(pl.multiple_of(h * half, half), half), :],
                preferred_element_type=jnp.float32,
            )

    def own_pair(i):
        return i // 2, i % 2

    def early(i):
        return 2 + i, i // 2

    def late(i):
        return 2 + i, 1 - i // 2

    score_scale = LOG2E / math.sqrt(HEAD_DIM)
    features = depth * 8

    def exchange(p, k, which):
        first, count = pieces[p]
        if which == 0:
            ref = keys.at[z, pl.ds(first, count), :]
        else:
            ref = values.at[z, pl.ds(0, HEAD_DIM), pl.ds(first, count)]
        return remote(ref, ref, kv_send.at[p, k, which], kv_recv.at[p, z, which], {"cp": others[k]})

    def arrived(p, owner):
        first, count = pieces[p]
        refs = (
            keys.at[owner, pl.ds(first, count), :],
            values.at[owner, pl.ds(0, HEAD_DIM), pl.ds(first, count)],
        )
        for which, ref in enumerate(refs):
            remote(
                ref, ref, kv_send.at[p, 0, which], kv_recv.at[p, owner, which], {"cp": others[0]}
            ).wait_recv()

    def turner(first, j, sub):
        start = starts[order_ref[2 * z + first // block]]
        at = pl.ds(pl.multiple_of(first % block + j * sub, sub), sub)
        cosine = turns[0, at, :] * start[0:1, :] - turns[1, at, :] * start[1:2, :]
        sine = turns[1, at, :] * start[2:3, :] + turns[0, at, :] * start[3:4, :]
        even = lax.rem(lax.broadcasted_iota(jnp.int32, (sub, HEAD_DIM), 1), 2) == 0

        def turned(content):
            later = pltpu.roll(content, HEAD_DIM - 1, 1)
            former = pltpu.roll(content, 1, 1)
            return content * cosine + jnp.where(even, later, former) * sine

        return turned

    def rate_of(at):
        return lax.rsqrt(squares[at, :] * (1.0 / features) + norm_epsilon)

    def finish_keys(p):
        first, count = pieces[p]

        @pl.loop(0, count // 128)
        def _(j):
            at = pl.ds(pl.multiple_of(first + j * 128, 128), 128)
            rate = rate_of(at)
            turned = turner(first, j, 128)
            keys[z, at, :] = turned(acc[at, q_cols : q_cols + k_cols] * rate).astype(jnp.bfloat16)
            value = acc[at, q_cols + k_cols : kv_end] * rate
            values[z, :HEAD_DIM, at] = jnp.transpose(value).astype(jnp.bfloat16)

        for k in (2, 1, 0):
            for which in (0, 1):
                exchange(p, k, which).start()

    def finish_queries(p):
        first, count = pieces[p]

        @pl.loop(0, count // 64)
        def _(j):
            at = pl.ds(pl.multiple_of(first + j * 64, 64), 64)
            rate = rate_of(at) * score_scale
            turned = turner(first, j, 64)
            for h in range(heads):
                cols = pl.ds(h * HEAD_DIM, HEAD_DIM)
                queries[at, cols] = turned(acc[at, cols] * rate).astype(jnp.bfloat16)

    def visible(s, owner, j):
        ahead = order_ref[2 * z + s] - order_ref[2 * owner + j]
        return jnp.where(ahead > 0, 0.0, masked_score)

    def attend(s, owner, first, count, diagonal=False):
        q_at = pl.ds(s * block, block)
        shade = None if diagonal else visible(s, owner, first // block)

        def one_head(h, inner):
            cols = pl.ds(pl.multiple_of(h * HEAD_DIM, HEAD_DIM), HEAD_DIM)
            scores = lax.dot_general(
                keys[owner, pl.ds(first, count), :], queries[q_at, cols],
                (((1,), (1,)), ((), ())), preferred_element_type=jnp.float32,
            )
            slot = s * heads + h
            extended = values[owner, :, pl.ds(first, count)]
            if diagonal:
                key_at = lax.broadcasted_iota(jnp.int32, (count, block), 0)
                query_at = lax.broadcasted_iota(jnp.int32, (count, block), 1)
                scores = jnp.where(key_at <= query_at, scores, masked_score)
                new_top = jnp.max(scores, axis=0, keepdims=True)
                share = jnp.exp2(scores - new_top).astype(jnp.bfloat16)
                weighted[slot] = jnp.dot(extended, share, preferred_element_type=jnp.float32)
            else:
                old_top = top[slot]
                new_top = jnp.maximum(old_top, jnp.max(scores, axis=0, keepdims=True) + shade)
                share = jnp.exp2(scores - (new_top - shade)).astype(jnp.bfloat16)
                weighted[slot] = weighted[slot] * jnp.exp2(old_top - new_top) + jnp.dot(
                    extended, share, preferred_element_type=jnp.float32
                )
            top[slot] = new_top
            return inner

        lax.fori_loop(0, heads, one_head, 0, unroll=2)

    def attend_others(s, p, wait):
        first, count = pieces[p]

        @pl.loop(0, 3)
        def _(k):
            owner = ring(k)
            if wait:
                arrived(p, owner)
            attend(s, owner, first, count)

    def finish_heads(s):
        at = pl.ds(s * block, block)
        for h in range(heads):
            slot = s * heads + h
            totals = weighted[slot, HEAD_DIM : HEAD_DIM + 1, :]
            part = weighted[slot, :HEAD_DIM, :] * (1.0 / totals)
            attended[at, h * HEAD_DIM : (h + 1) * HEAD_DIM] = jnp.transpose(part).astype(
                jnp.bfloat16
            )
            norm_ref[h : h + 1, at] = (top[slot] + jnp.log2(totals)) * (1.0 / LOG2E)

    weights_of(0, 1)
    landed(0, "s0", "s1")
    process(*pieces[0], 4, own_pair)
    landed(0, "dx0")
    send(0, "fy", "a0")
    landed(0, "dy1")
    send(0, "fx", "b1")
    send(1, "dx0", "dy1", "dx1", "dy0")
    send(2, "dx0", "dy1")
    for copy in o_copies.values():
        copy.start()
    weights_of(2, 3, 4, 5)
    landed(0, "a0", "b1")
    process(*pieces[0], 4, early)
    landed(0, "dx1")
    send(0, "a1")
    landed(0, "dy0")
    send(0, "b0")
    for p in (1, 2):
        landed(p, "s0", "s1")
    process(block, block, 4, own_pair)
    landed(0, "a1", "b0")
    process(*pieces[0], 4, late)
    weights_of(6, 7)
    landed(0, "fy")
    send(0, "c0")
    landed(0, "fx")
    send(0, "c1")
    process(*pieces[0], 2, lambda i: (6, i))
    landed(0, "c0", "c1")
    process(*pieces[0], 2, lambda i: (7, i))
    small[1].wait()
    small[2].wait()
    finish_keys(0)
    landed(1, "dx0")
    send(1, "fy", "a0")
    landed(1, "dy1")
    send(1, "fx", "b1")
    send(2, "dx1", "dy0")
    finish_queries(0)
    attend(0, z, 0, block, diagonal=True)
    landed(1, "a0", "b1")
    process(*pieces[1], 4, early)
    landed(1, "dx1")
    send(1, "a1")
    landed(1, "dy0")
    send(1, "b0")
    landed(1, "a1", "b0")
    process(*pieces[1], 4, late)
    landed(2, "dx0")
    send(2, "fy", "a0")
    landed(2, "dy1")
    send(2, "fx", "b1")
    landed(2, "a0", "b1")
    process(*pieces[2], 4, early)
    landed(1, "fy")
    send(1, "c0")
    landed(1, "fx")
    send(1, "c1")
    process(*pieces[1], 2, lambda i: (6, i))
    landed(1, "c0", "c1")
    process(*pieces[1], 2, lambda i: (7, i))
    finish_keys(1)
    finish_queries(1)
    landed(2, "dx1")
    send(2, "a1")
    landed(2, "dy0")
    send(2, "b0")
    landed(2, "a1", "b0")
    process(*pieces[2], 4, late)
    landed(2, "fy")
    send(2, "c0")
    landed(2, "fx")
    send(2, "c1")
    process(*pieces[2], 2, lambda i: (6, i))
    landed(2, "c0", "c1")
    process(*pieces[2], 2, lambda i: (7, i))
    finish_keys(2)
    finish_queries(2)

    attend(0, z, block, block)
    attend(1, z, block, block, diagonal=True)
    attend(1, z, 0, block)
    attend_others(0, 0, True)
    attend_others(1, 0, False)
    attend_others(0, 1, True)
    attend_others(1, 1, False)
    for p in range(3):
        for copy in gather[p].values():
            copy.wait_send()
    attend_others(0, 2, True)
    finish_heads(0)

    scatter = []
    for s in range(2):
        at = pl.ds(s * block, block)
        plan = {}
        for e in (1, 3, 5, 7):
            for h in range(2):
                plan["s", e, h] = (held.at[e, h, at, :], from_sib.at[e // 2, h, at, :], sib)
        plan["six", 0] = (held.at[6, 0, at, :], from_six.at[0, at, :], nx)
        plan["six", 1] = (held.at[6, 1, at, :], from_six.at[1, at, :], ny)
        for h in range(2):
            plan["x", h] = (held.at[2, h, at, :], from_x.at[h, at, :], nx)
            plan["y", h] = (held.at[4, h, at, :], from_y.at[h, at, :], ny)
        scatter.append(
            {
                name: remote(source, target, rs_send.at[s, i], rs_recv.at[s, i], {"tp": other})
                for i, (name, (source, target, other)) in enumerate(plan.items())
            }
        )

    def term(s, e, h):
        if s == 0:
            o_copies[e, h].wait()
        at = pl.ds(s * block, block)
        held[e, h, at, :] = jnp.dot(
            attended[at, :], out_weights[e, h], preferred_element_type=jnp.float32
        ).astype(jnp.bfloat16)
        if e % 2:
            scatter[s]["s", e, h].start()

    def summed(s, e, h, more=()):
        scatter[s]["s", e + 1, h].wait_recv()

        @pl.loop(0, block // 64)
        def _(i):
            at = pl.ds(pl.multiple_of(s * block + i * 64, 64), 64)
            total = held[e, h, at, :].astype(jnp.float32)
            total = total + from_sib[e // 2, h, at, :].astype(jnp.float32)
            for other in more:
                total = total + other[at, :].astype(jnp.float32)
            if e:
                held[e, h, at, :] = total.astype(jnp.bfloat16)
            else:
                out_ref[at, h * half : (h + 1) * half] = total.astype(jnp.bfloat16)

    def far(s):
        term(s, 7, 0)
        term(s, 6, 0)
        term(s, 7, 1)
        summed(s, 6, 0)
        scatter[s]["six", 0].start()
        term(s, 6, 1)
        term(s, 3, 0)
        summed(s, 6, 1)
        scatter[s]["six", 1].start()
        term(s, 2, 0)
        term(s, 5, 1)
        summed(s, 2, 0)
        scatter[s]["x", 0].start()
        term(s, 4, 1)
        term(s, 3, 1)
        summed(s, 4, 1)
        scatter[s]["y", 1].start()

    def near(s):
        term(s, 2, 1)
        term(s, 5, 0)
        term(s, 4, 0)
        scatter[s]["six", 0].wait_recv()
        summed(s, 4, 0, (from_six.at[0],))
        scatter[s]["y", 0].start()
        scatter[s]["six", 1].wait_recv()
        summed(s, 2, 1, (from_six.at[1],))
        scatter[s]["x", 1].start()

    def last(s):
        for h in range(2):
            scatter[s]["x", h].wait_recv()
            scatter[s]["y", h].wait_recv()
            summed(s, 0, h, (from_x.at[h], from_y.at[h]))

    far(0)
    attend_others(1, 2, False)
    finish_heads(1)
    near(0)
    far(1)
    for s in range(2):
        for h in range(2):
            term(s, 1, h)
            term(s, 0, h)
    near(1)
    last(0)
    last(1)
    for p in range(3):
        for k in range(3):
            for which in range(2):
                exchange(p, k, which).wait_send()
    for s in range(2):
        for copy in scatter[s].values():
            copy.wait_send()


def rotary_tables(block, count):
    lanes = np.arange(HEAD_DIM)
    rates = rope_base ** (-2.0 * (lanes // 2) / HEAD_DIM)
    sign = np.where(lanes % 2 == 0, -1.0, 1.0)
    inside = np.arange(block)[:, None] * rates[None, :]
    turns = np.stack([np.cos(inside), np.sin(inside)]).astype(np.float32)
    begin = (np.arange(count) * block)[:, None] * rates[None, :]
    cosine, sine = np.cos(begin), np.sin(begin)
    starts = np.stack([cosine, sine, sign * cosine, sign * sine], axis=1)
    starts = np.concatenate([starts, np.zeros_like(starts)], axis=1).astype(np.float32)
    return jnp.asarray(turns), jnp.asarray(starts)


def fused_shards(
    n_cp, n_tp, checkpoint, norm_gain, query_weight, key_weight, value_weight, output_weight, block_order
):
    rows, depth = checkpoint.shape
    q_cols = query_weight.shape[1]
    k_cols = key_weight.shape[1]
    heads = q_cols // HEAD_DIM
    block = rows // 2
    half = depth // 2
    bf16, f32 = jnp.bfloat16, jnp.float32
    turns, starts = rotary_tables(block, block_order.shape[0])
    any_spec = pl.BlockSpec(memory_space=pl.ANY)
    vmem = pl.BlockSpec(memory_space=pltpu.VMEM)
    smem = pl.BlockSpec(memory_space=pltpu.SMEM)
    dma = pltpu.SemaphoreType.DMA
    return pl.pallas_call(
        layer_kernel,
        out_shape=(
            jax.ShapeDtypeStruct((rows, depth), bf16),
            jax.ShapeDtypeStruct((heads, rows), f32),
        ),
        in_specs=[smem] + [any_spec] * 8,
        out_specs=(vmem, vmem),
        scratch_shapes=[
            pltpu.VMEM((8, 2, rows, half), bf16),
            pltpu.VMEM((8, depth, q_cols + 2 * k_cols), bf16),
            pltpu.VMEM((8, 2, q_cols, half), bf16),
            pltpu.VMEM((8, 2, 1, half), f32),
            pltpu.VMEM((rows, q_cols + 2 * k_cols), f32),
            pltpu.VMEM((block, half), bf16),
            pltpu.VMEM((rows, 1), f32),
            pltpu.VMEM((2, block, HEAD_DIM), f32),
            pltpu.VMEM(starts.shape, f32),
            pltpu.VMEM((rows, q_cols), bf16),
            pltpu.VMEM((n_cp, rows, HEAD_DIM), bf16),
            pltpu.VMEM((n_cp, HEAD_DIM + 16, rows), bf16),
            pltpu.VMEM((2 * heads, HEAD_DIM + 16, block), f32),
            pltpu.VMEM((2 * heads, 1, block), f32),
            pltpu.VMEM((rows, q_cols), bf16),
            pltpu.VMEM((4, 2, rows, half), bf16),
            pltpu.VMEM((2, rows, half), bf16),
            pltpu.VMEM((2, rows, half), bf16),
            pltpu.VMEM((2, rows, half), bf16),
            dma((2, 2)),
            dma((8, 3)),
            dma((8, 2)),
            dma((3,)),
            dma((3, 14)),
            dma((3, 14)),
            dma((3, n_cp - 1, 2)),
            dma((3, n_cp, 2)),
            dma((2, 14)),
            dma((2, 14)),
        ],
        compiler_params=pltpu.CompilerParams(
            collective_id=0, has_side_effects=True, vmem_limit_bytes=FUSED_BYTES
        ),
        name="layer",
    )(
        block_order, checkpoint, norm_gain.reshape(8, 2, 1, half), query_weight, key_weight,
        value_weight, output_weight, turns, starts,
    )


def shards(
    n_cp, n_tp, checkpoint, norm_gain, query_weight, key_weight, value_weight, output_weight, block_order
):
    rows = checkpoint.shape[0]
    q_cols = query_weight.shape[1]
    heads = q_cols // HEAD_DIM
    block = rows // 2
    context_rank = lax.axis_index("cp")
    own_blocks = lax.dynamic_slice_in_dim(block_order, 2 * context_rank, 2)
    offsets = jnp.arange(block, dtype=jnp.int32)
    positions = (own_blocks[:, None] * block + offsets[None, :]).reshape(rows)

    vmem = pl.BlockSpec(memory_space=pltpu.VMEM)
    smem = pl.BlockSpec(memory_space=pltpu.SMEM)
    bf16, f32 = jnp.bfloat16, jnp.float32
    dma = pltpu.SemaphoreType.DMA
    queries, key_value = project_any(
        checkpoint, norm_gain, query_weight, key_weight, value_weight, positions
    )
    attended, normalizer = pl.pallas_call(
        functools.partial(attend_kernel, n_cp),
        out_shape=(
            jax.ShapeDtypeStruct((rows, q_cols), bf16),
            jax.ShapeDtypeStruct((heads, rows), f32),
        ),
        in_specs=[smem, vmem, pl.BlockSpec(memory_space=pl.ANY)],
        out_specs=(vmem, vmem),
        scratch_shapes=[
            pltpu.VMEM((n_cp, rows, 2 * HEAD_DIM), bf16),
            pltpu.VMEM((rows, 2 * HEAD_DIM), bf16),
            pltpu.VMEM((rows, rows), f32),
            pltpu.VMEM((heads, rows, 1), f32),
            pltpu.VMEM((heads, rows, 2 * HEAD_DIM), f32),
            pltpu.VMEM((rows, HEAD_DIM), f32),
            dma,
            dma((n_cp - 1, 2)),
            dma((n_cp - 1, 2)),
        ],
        compiler_params=pltpu.CompilerParams(
            collective_id=1, has_side_effects=True, vmem_limit_bytes=VMEM_BYTES
        ),
        name="attend",
    )(block_order, queries, key_value)
    partial_terms = jnp.dot(attended, output_weight, preferred_element_type=jnp.float32)
    projected = lax.psum_scatter(partial_terms.astype(bf16), "tp", scatter_dimension=1, tiled=True)
    return (projected, normalizer)


def solution(mesh):
    n_cp, n_tp = mesh.shape["cp"], mesh.shape["tp"]
    body = fused_shards if (n_cp, n_tp) == (4, 8) else shards
    return jax.shard_map(
        functools.partial(body, n_cp, n_tp),
        mesh=mesh,
        in_specs=(
            P("cp", "tp"),
            P(),
            P(None, "tp"),
            P(None, "tp"),
            P(None, "tp"),
            P("tp", None),
            P(),
        ),
        out_specs=(P("cp", "tp"), P("tp", "cp")),
        check_vma=False,
    )
```

```python
import functools
import math

import jax
import jax.numpy as jnp
import numpy as np
from jax import lax
from jax.experimental import pallas as pl
from jax.experimental.pallas import tpu as pltpu
from jax.sharding import PartitionSpec as P

HEAD_DIM = 128
KV_HEADS = 8
MESH = pl.DeviceIdType.MESH
VMEM_BYTES = 62 * 1024 * 1024
FUSED_BYTES = 67_000_000

rope_base = 500000.0
norm_epsilon = 1e-05
masked_score = -1e30
LOG2E = 1.4426950408889634


def partner_2(block, axis, stride):
    count = lax.axis_size(axis)
    route = []
    for low in range(count):
        high = low | 1 << stride
        if high != low and high < count:
            route += [(low, high), (high, low)]
    return lax.ppermute(block, axis, route)


def turn_pairs(matrix, positions, first_pair):
    pair_count = matrix.shape[-1] // 2
    pair_index = (first_pair + jnp.arange(pair_count, dtype=jnp.int32)).astype(jnp.float32)
    inverse_rates = rope_base ** (-2.0 * pair_index / HEAD_DIM)
    angles = positions.astype(jnp.float32)[:, None] * inverse_rates[None, :]
    cosine = jnp.cos(angles)[:, None, :]
    sine_part = jnp.sin(angles)[:, None, :]
    paired = matrix.reshape(matrix.shape[0], matrix.shape[1], pair_count, 2)
    former = paired[..., 0]
    latter = paired[..., 1]
    turned = jnp.stack(
        [former * cosine - latter * sine_part, former * sine_part + latter * cosine], axis=-1
    )
    return turned.reshape(matrix.shape)


def project_any(checkpoint, norm_gain, query_weight, key_weight, value_weight, positions):
    rows = checkpoint.shape[0]
    heads = query_weight.shape[1] // HEAD_DIM
    key_columns = key_weight.shape[1]
    gathered = lax.all_gather(checkpoint, "tp", axis=1, tiled=True)
    widened = gathered.astype(jnp.float32)
    mean_square = jnp.mean(widened * widened, axis=-1, keepdims=True)
    normed = (widened * lax.rsqrt(mean_square + norm_epsilon) * norm_gain).astype(jnp.bfloat16)
    query_features = jnp.dot(normed, query_weight, preferred_element_type=jnp.float32)
    key_features = jnp.dot(normed, key_weight, preferred_element_type=jnp.float32)
    value_features = jnp.dot(normed, value_weight, preferred_element_type=jnp.float32)
    turned = turn_pairs(query_features.reshape(rows, heads, HEAD_DIM), positions, 0)
    queries = (turned * (LOG2E / math.sqrt(HEAD_DIM))).astype(jnp.bfloat16)
    sharing = lax.axis_size("tp") // KV_HEADS
    part_of_head = lax.axis_index("tp") % sharing
    key_part = turn_pairs(
        key_features.reshape(rows, 1, key_columns), positions, part_of_head * (key_columns // 2)
    )
    key_part = key_part.astype(jnp.bfloat16).reshape(rows, key_columns)
    own_pair = jnp.stack([key_part, value_features.astype(jnp.bfloat16)])
    key_value = own_pair
    if sharing == 2:
        partner = partner_2(own_pair, "tp", 0)
        lower_first = jnp.concatenate([own_pair, partner], axis=-1)
        upper_first = jnp.concatenate([partner, own_pair], axis=-1)
        key_value = jnp.where(part_of_head == 0, lower_first, upper_first)
    return (
        queries.reshape(rows, heads * HEAD_DIM),
        jnp.concatenate([key_value[0], key_value[1]], axis=-1),
    )


def flipped(me, offset):
    result = me
    for bit in (1, 2, 4):
        chosen = offset // bit % 2
        result = result + chosen * (bit - 2 * bit * (me // bit % 2))
    return result


def greet(axis, others):
    barrier = pltpu.get_barrier_semaphore()
    for other in others:
        pl.semaphore_signal(barrier, inc=1, device_id={axis: other}, device_id_type=MESH)
    pl.semaphore_wait(barrier, len(others))


def attend_kernel(
    n_cp, order_ref, q_ref, kv_hbm, out_ref, norm_ref,
    ring, extended, bias, top, weighted, norms, kv_sem, send_sems, recv_sems,
):
    me = lax.axis_index("cp")
    rows = q_ref.shape[0]
    block = rows // 2
    heads = q_ref.shape[1] // HEAD_DIM
    right, left = lax.rem(me + 1, n_cp), lax.rem(me + n_cp - 1, n_cp)
    own_copy = pltpu.make_async_copy(kv_hbm, ring.at[0], kv_sem)
    own_copy.start()
    greet("cp", (right, left))
    own_copy.wait()

    def hop(step, h):
        at = pl.ds(h * block, block)
        return pltpu.make_async_remote_copy(
            src_ref=ring.at[step, at, :],
            dst_ref=ring.at[step + 1, at, :],
            send_sem=send_sems.at[step, h],
            recv_sem=recv_sems.at[step, h],
            device_id={"cp": right},
            device_id_type=MESH,
        )

    hop(0, 0).start()
    hop(0, 1).start()
    extended[:, HEAD_DIM:] = jnp.ones((rows, HEAD_DIM), jnp.bfloat16)
    top[...] = jnp.full(top.shape, masked_score, jnp.float32)
    weighted[...] = jnp.zeros_like(weighted)

    def visit(step, carried):
        for h in range(2):

            @pl.when(step > 0)
            def _():
                hop(step - 1, h).wait_recv()

            @pl.when(jnp.logical_and(step > 0, step < n_cp - 1))
            def _():
                hop(step, h).start()

        owner = lax.rem(me - step + n_cp, n_cp)
        extended[:, :HEAD_DIM] = ring[step, :, HEAD_DIM:]
        base = lax.broadcasted_iota(jnp.int32, (block, block), 0) - lax.broadcasted_iota(
            jnp.int32, (block, block), 1
        )
        for i in range(2):
            for j in range(2):
                ahead = (order_ref[2 * me + i] - order_ref[2 * owner + j]) * block
                bias[i * block : (i + 1) * block, j * block : (j + 1) * block] = jnp.where(
                    base + ahead >= 0, 0.0, masked_score
                )

        def one_head(h, inner):
            cols = pl.ds(pl.multiple_of(h * HEAD_DIM, HEAD_DIM), HEAD_DIM)
            keys = ring[step, :, :HEAD_DIM]
            for i in range(2):
                at = pl.ds(i * block, block)
                scores = lax.dot_general(
                    q_ref[at, cols], keys, (((1,), (1,)), ((), ())),
                    preferred_element_type=jnp.float32,
                )
                scores = scores + bias[at, :]
                old_top = top[h, at, :]
                new_top = jnp.maximum(old_top, jnp.max(scores, axis=1, keepdims=True))
                weights = jnp.exp2(scores - new_top).astype(jnp.bfloat16)
                shrink = jnp.exp2(old_top - new_top)
                top[h, at, :] = new_top
                weighted[h, at, :] = weighted[h, at, :] * shrink + jnp.dot(
                    weights, extended[...], preferred_element_type=jnp.float32
                )
            return inner

        lax.fori_loop(0, heads, one_head, 0, unroll=2)
        return carried

    lax.fori_loop(0, n_cp, visit, 0)
    lane = lax.broadcasted_iota(jnp.int32, (rows, HEAD_DIM), 1)
    norms[...] = jnp.zeros_like(norms)
    for h in range(heads):
        totals = weighted[h, :, HEAD_DIM:]
        out_ref[:, h * HEAD_DIM : (h + 1) * HEAD_DIM] = (
            weighted[h, :, :HEAD_DIM] / totals
        ).astype(jnp.bfloat16)
        norm = (top[h] + jnp.log2(totals)) * (1.0 / LOG2E)
        norms[...] = jnp.where(lane == h, norm, norms[...])
    norm_ref[...] = jnp.transpose(norms[...])[:heads, :]

    for step in range(n_cp - 1):
        for h in range(2):
            hop(step, h).wait_send()


def layer_kernel(
    order_ref, x_hbm, gain_hbm, wq_hbm, wk_hbm, wv_hbm, wo_hbm, turns_hbm, starts_hbm,
    out_ref, norm_ref,
    held, weights, out_weights, gains, acc, scaled, squares, turns, starts,
    queries, keys, values, weighted, top, from_sib, from_six, from_x, from_y,
    x_sems, w_sems, o_sems, t_sems, ag_send, ag_recv, kv_send, kv_recv, rs_send, rs_recv,
):
    me = lax.axis_index("tp")
    z = lax.axis_index("cp")
    rows, depth = x_hbm.shape
    half = depth // 2
    block = rows // 2
    q_cols = wq_hbm.shape[1]
    k_cols = wk_hbm.shape[1]
    heads = q_cols // HEAD_DIM
    kv_end = q_cols + 2 * k_cols
    sib, nx, ny = flipped(me, 1), flipped(me, 2), flipped(me, 4)
    pieces = ((0, block), (block, block // 2), (block + block // 2, block // 2))

    upper = z // 2
    low = z + upper * (3 - 2 * z)
    others = []
    for k in range(3):
        near = k + 1 - (low if k == 0 else 0)
        others.append(near + upper * (3 - 2 * near))

    x_copies = []
    for p, (first, count) in enumerate(((0, block), (block, block))):
        for h in range(2):
            at = pl.ds(first, count)
            x_copies.append(
                pltpu.make_async_copy(
                    x_hbm.at[at, pl.ds(h * half, half)], held.at[0, h, at, :], x_sems.at[p, h]
                )
            )
    for copy in x_copies:
        copy.start()
    small = [
        pltpu.make_async_copy(gain_hbm, gains, t_sems.at[0]),
        pltpu.make_async_copy(turns_hbm, turns, t_sems.at[1]),
        pltpu.make_async_copy(starts_hbm, starts, t_sems.at[2]),
    ]
    small[0].start()
    w_copies = []
    for e in range(8):
        chunk = pl.ds(pl.multiple_of(flipped(me, e) * depth, depth), depth)
        parts = ((wq_hbm, 0, q_cols), (wk_hbm, q_cols, k_cols), (wv_hbm, q_cols + k_cols, k_cols))
        w_copies.append(
            [
                pltpu.make_async_copy(
                    w.at[chunk, :], weights.at[e, :, pl.ds(at, size)], w_sems.at[e, i]
                )
                for i, (w, at, size) in enumerate(parts)
            ]
        )
    o_copies = {}
    for e in (7, 6, 3, 2, 5, 4, 1, 0):
        for h in range(2):
            at = pl.ds(pl.multiple_of(flipped(me, e) * depth + h * half, half), half)
            o_copies[e, h] = pltpu.make_async_copy(
                wo_hbm.at[:, at], out_weights.at[e, h], o_sems.at[e, h]
            )

    barrier = pltpu.get_barrier_semaphore()
    peers = [{"tp": sib}, {"tp": nx}, {"tp": ny}] + [{"cp": other} for other in others]
    for peer in peers:
        pl.semaphore_signal(barrier, inc=1, device_id=peer, device_id_type=MESH)
    pl.semaphore_wait(barrier, len(peers))

    def remote(source, target, send, recv, device):
        return pltpu.make_async_remote_copy(
            src_ref=source, dst_ref=target, send_sem=send, recv_sem=recv,
            device_id=device, device_id_type=MESH,
        )

    gather = []
    for p, (first, count) in enumerate(pieces):
        at = pl.ds(first, count)

        def part(slot, h, at=at):
            return held.at[slot, h, at, :]

        plan = {
            "dx0": (0, 0, 2, nx), "dx1": (0, 1, 2, nx), "dy0": (0, 0, 4, ny), "dy1": (0, 1, 4, ny),
            "s0": (0, 0, 1, sib), "s1": (0, 1, 1, sib), "fy": (2, 0, 6, ny), "fx": (4, 1, 6, nx),
            "a0": (2, 0, 3, sib), "a1": (2, 1, 3, sib), "b0": (4, 0, 5, sib), "b1": (4, 1, 5, sib),
            "c0": (6, 0, 7, sib), "c1": (6, 1, 7, sib),
        }
        gather.append(
            {
                name: remote(
                    part(slot, h), part(to, h), ag_send.at[p, i], ag_recv.at[p, i], {"tp": other}
                )
                for i, (name, (slot, h, to, other)) in enumerate(plan.items())
            }
        )

    def send(p, *names):
        for name in names:
            gather[p][name].start()

    def landed(p, *names):
        for name in names:
            gather[p][name].wait_recv()

    for copy in x_copies[:2]:
        copy.wait()
    send(0, "dx0", "dy1", "dx1", "dy0", "s0", "s1")
    for copies in w_copies:
        for copy in copies:
            copy.start()
    small[1].start()
    small[2].start()
    acc[...] = jnp.zeros_like(acc)
    squares[...] = jnp.zeros_like(squares)
    values[:, HEAD_DIM:, :] = jnp.ones((4, 16, rows), jnp.bfloat16)
    for copy in x_copies[2:]:
        copy.wait()
    for p in (1, 2):
        send(p, "s0", "s1")
    small[0].wait()

    def weights_of(*slots):
        for e in slots:
            for copy in w_copies[e]:
                copy.wait()

    def process(first, count, chunks, chunk_of):
        @pl.loop(0, chunks)
        def _(i):
            e, h = chunk_of(i)
            source = flipped(me, e)

            @pl.loop(0, count // 64)
            def _(j):
                at = pl.ds(pl.multiple_of(first + j * 64, 64), 64)
                into = pl.ds(pl.multiple_of(j * 64, 64), 64)
                wide = held[e, h, at, :].astype(jnp.float32)
                squares[at, :] += jnp.sum(wide * wide, axis=1, keepdims=True)
                scaled[into, :] = (wide * gains[source, h]).astype(jnp.bfloat16)

            acc[first : first + count, :] += jnp.dot(
                scaled[:count, :],
                weights[e, pl.ds(pl.multiple_of(h * half, half), half), :],
                preferred_element_type=jnp.float32,
            )

    def own_pair(i):
        return i // 2, i % 2

    def early(i):
        return 2 + i, i // 2

    def late(i):
        return 2 + i, 1 - i // 2

    score_scale = LOG2E / math.sqrt(HEAD_DIM)
    features = depth * 8

    def exchange(p, k, which):
        first, count = pieces[p]
        if which == 0:
            ref = keys.at[z, pl.ds(first, count), :]
        else:
            ref = values.at[z, pl.ds(0, HEAD_DIM), pl.ds(first, count)]
        return remote(ref, ref, kv_send.at[p, k, which], kv_recv.at[p, z, which], {"cp": others[k]})

    def arrived(p, owner):
        first, count = pieces[p]
        refs = (
            keys.at[owner, pl.ds(first, count), :],
            values.at[owner, pl.ds(0, HEAD_DIM), pl.ds(first, count)],
        )
        for which, ref in enumerate(refs):
            remote(
                ref, ref, kv_send.at[p, 0, which], kv_recv.at[p, owner, which], {"cp": others[0]}
            ).wait_recv()

    def turner(first, j, sub):
        start = starts[order_ref[2 * z + first // block]]
        at = pl.ds(pl.multiple_of(first % block + j * sub, sub), sub)
        cosine = turns[0, at, :] * start[0:1, :] - turns[1, at, :] * start[1:2, :]
        sine = turns[1, at, :] * start[2:3, :] + turns[0, at, :] * start[3:4, :]
        even = lax.rem(lax.broadcasted_iota(jnp.int32, (sub, HEAD_DIM), 1), 2) == 0

        def turned(content):
            later = pltpu.roll(content, HEAD_DIM - 1, 1)
            former = pltpu.roll(content, 1, 1)
            return content * cosine + jnp.where(even, later, former) * sine

        return turned

    def rate_of(at):
        return lax.rsqrt(squares[at, :] * (1.0 / features) + norm_epsilon)

    def finish_keys(p):
        first, count = pieces[p]

        @pl.loop(0, count // 128)
        def _(j):
            at = pl.ds(pl.multiple_of(first + j * 128, 128), 128)
            rate = rate_of(at)
            turned = turner(first, j, 128)
            keys[z, at, :] = turned(acc[at, q_cols : q_cols + k_cols] * rate).astype(jnp.bfloat16)
            value = acc[at, q_cols + k_cols : kv_end] * rate
            values[z, :HEAD_DIM, at] = jnp.transpose(value).astype(jnp.bfloat16)

        for k in (2, 1, 0):
            for which in (0, 1):
                exchange(p, k, which).start()

    def finish_queries(p):
        first, count = pieces[p]

        @pl.loop(0, count // 64)
        def _(j):
            at = pl.ds(pl.multiple_of(first + j * 64, 64), 64)
            rate = rate_of(at) * score_scale
            turned = turner(first, j, 64)
            for h in range(heads):
                cols = pl.ds(h * HEAD_DIM, HEAD_DIM)
                queries[at, cols] = turned(acc[at, cols] * rate).astype(jnp.bfloat16)

    def visible(s, owner, j):
        ahead = order_ref[2 * z + s] - order_ref[2 * owner + j]
        return jnp.where(ahead > 0, 0.0, masked_score)

    def attend(s, chunks, together, start=False, finish=False):
        q_at = pl.ds(s * block, block)
        shades = {}
        for chunk in chunks:
            for owner, first, count, diagonal in chunk:
                if not diagonal:
                    shades[id(owner), first] = visible(s, owner, first // block)

        def columns(h):
            return pl.ds(pl.multiple_of(h * HEAD_DIM, HEAD_DIM), HEAD_DIM)

        def scored(h, side, j, peak):
            offset = side * block
            for owner, first, count, diagonal in chunks[j]:
                scores = lax.dot_general(
                    keys[owner, pl.ds(first, count), :], queries[q_at, columns(h)],
                    (((1,), (1,)), ((), ())), preferred_element_type=jnp.float32,
                )
                if diagonal:
                    key_at = lax.broadcasted_iota(jnp.int32, (count, block), 0)
                    query_at = lax.broadcasted_iota(jnp.int32, (count, block), 1)
                    scores = jnp.where(key_at <= query_at, scores, masked_score)
                acc[offset : offset + count, j * block : (j + 1) * block] = scores
                offset += count
                highest = jnp.max(scores, axis=0, keepdims=True)
                if not diagonal:
                    highest = highest + shades[id(owner), first]
                peak = highest if peak is None else jnp.maximum(peak, highest)
            return peak

        def beside(coming, side, h, peak):
            slot = s * heads + h
            new_top = peak
            if not start:
                old_top = top[slot]
                new_top = jnp.maximum(old_top, peak)
                shrink = jnp.exp2(old_top - new_top)
            next_peak, total = None, None
            for j, chunk in enumerate(chunks):
                if coming is not None:
                    next_peak = scored(coming, 1 - side, j, next_peak)
                offset = side * block
                shares, extended = [], []
                for owner, first, count, diagonal in chunk:
                    lean = new_top if diagonal else new_top - shades[id(owner), first]
                    scores = acc[offset : offset + count, j * block : (j + 1) * block]
                    shares.append(jnp.exp2(scores - lean).astype(jnp.bfloat16))
                    extended.append(values[owner, :, pl.ds(first, count)])
                    offset += count
                share, wide = shares[0], extended[0]
                if len(chunk) > 1:
                    share, wide = jnp.concatenate(shares, 0), jnp.concatenate(extended, 1)
                piece = jnp.dot(wide, share, preferred_element_type=jnp.float32)
                total = piece if total is None else total + piece
            if not start:
                total = weighted[slot] * shrink + total
            if finish:
                sums = total[HEAD_DIM : HEAD_DIM + 1, :]
                part = total[:HEAD_DIM, :] * (1.0 / sums)
                queries[q_at, columns(h)] = jnp.transpose(part).astype(jnp.bfloat16)
                norm_ref[pl.ds(h, 1), q_at] = (new_top + jnp.log2(sums)) * (1.0 / LOG2E)
            else:
                weighted[slot] = total
                top[slot] = new_top
            return next_peak

        peak = None
        for j in range(len(chunks)):
            peak = scored(0, 0, j, peak)
        if together == heads:
            for h in range(heads):
                peak = beside(h + 1 if h + 1 < heads else None, h % 2, h, peak)
        else:

            def group(i, peak):
                for u in range(together):
                    h = i * together + u
                    coming = h + 1 if u + 1 < together else jnp.minimum(h + 1, heads - 1)
                    peak = beside(coming, u % 2, h, peak)
                return peak

            lax.fori_loop(0, heads // together, group, peak)

    weights_of(0, 1)
    landed(0, "s0", "s1")
    process(*pieces[0], 4, own_pair)
    landed(0, "dx0")
    send(0, "fy", "a0")
    landed(0, "dy1")
    send(0, "fx", "b1")
    send(1, "dx0", "dy1", "dx1", "dy0")
    send(2, "dx0", "dy1")
    for copy in o_copies.values():
        copy.start()
    weights_of(2, 3, 4, 5)
    landed(0, "a0", "b1")
    process(*pieces[0], 4, early)
    landed(0, "dx1")
    send(0, "a1")
    landed(0, "dy0")
    send(0, "b0")
    for p in (1, 2):
        landed(p, "s0", "s1")
    process(block, block, 4, own_pair)
    landed(0, "a1", "b0")
    process(*pieces[0], 4, late)
    weights_of(6, 7)
    landed(0, "fy")
    send(0, "c0")
    landed(0, "fx")
    send(0, "c1")
    process(*pieces[0], 2, lambda i: (6, i))
    landed(0, "c0", "c1")
    process(*pieces[0], 2, lambda i: (7, i))
    small[1].wait()
    small[2].wait()
    finish_keys(0)
    landed(1, "dx0")
    send(1, "fy", "a0")
    landed(1, "dy1")
    send(1, "fx", "b1")
    send(2, "dx1", "dy0")
    finish_queries(0)
    landed(1, "a0", "b1")
    process(*pieces[1], 4, early)
    landed(1, "dx1")
    send(1, "a1")
    landed(1, "dy0")
    send(1, "b0")
    landed(1, "a1", "b0")
    process(*pieces[1], 4, late)
    landed(2, "dx0")
    send(2, "fy", "a0")
    landed(2, "dy1")
    send(2, "fx", "b1")
    landed(2, "a0", "b1")
    process(*pieces[2], 4, early)
    landed(1, "fy")
    send(1, "c0")
    landed(1, "fx")
    send(1, "c1")
    process(*pieces[1], 2, lambda i: (6, i))
    landed(1, "c0", "c1")
    process(*pieces[1], 2, lambda i: (7, i))
    finish_keys(1)
    finish_queries(1)
    landed(2, "dx1")
    send(2, "a1")
    landed(2, "dy0")
    send(2, "b0")
    landed(2, "a1", "b0")
    process(*pieces[2], 4, late)
    landed(2, "fy")
    send(2, "c0")
    landed(2, "fx")
    send(2, "c1")
    process(*pieces[2], 2, lambda i: (6, i))
    landed(2, "c0", "c1")
    process(*pieces[2], 2, lambda i: (7, i))
    finish_keys(2)
    finish_queries(2)

    for owner in others:
        arrived(0, owner)
    third = block // 2
    near, middle, distant = others
    whole = [[(owner, 0, block, False)] for owner in others]
    attend(0, [[(z, 0, block, True)]] + whole, 4, start=True)
    attend(1, [[(z, block, block, True)], [(z, 0, block, False)]] + whole, 4, start=True)
    for owner in others:
        arrived(1, owner)
    attend(
        0,
        [
            [(z, block, block, False)],
            [(near, block, third, False), (middle, block, third, False)],
            [(distant, block, third, False)],
        ],
        4,
    )
    for p in range(3):
        for copy in gather[p].values():
            copy.wait_send()
    for owner in others:
        arrived(2, owner)
    attend(
        0,
        [
            [(near, block + third, third, False), (middle, block + third, third, False)],
            [(distant, block + third, third, False)],
        ],
        heads,
        finish=True,
    )

    scatter = []
    for s in range(2):
        at = pl.ds(s * block, block)
        plan = {}
        for e in (1, 3, 5, 7):
            for h in range(2):
                plan["s", e, h] = (held.at[e, h, at, :], from_sib.at[e // 2, h, at, :], sib)
        plan["six", 0] = (held.at[6, 0, at, :], from_six.at[0, at, :], nx)
        plan["six", 1] = (held.at[6, 1, at, :], from_six.at[1, at, :], ny)
        for h in range(2):
            plan["x", h] = (held.at[2, h, at, :], from_x.at[h, at, :], nx)
            plan["y", h] = (held.at[4, h, at, :], from_y.at[h, at, :], ny)
        scatter.append(
            {
                name: remote(source, target, rs_send.at[s, i], rs_recv.at[s, i], {"tp": other})
                for i, (name, (source, target, other)) in enumerate(plan.items())
            }
        )

    def term(s, e, h):
        if s == 0:
            o_copies[e, h].wait()
        at = pl.ds(s * block, block)
        held[e, h, at, :] = jnp.dot(
            queries[at, :], out_weights[e, h], preferred_element_type=jnp.float32
        ).astype(jnp.bfloat16)
        if e % 2:
            scatter[s]["s", e, h].start()

    def summed(s, e, h, more=()):
        scatter[s]["s", e + 1, h].wait_recv()

        @pl.loop(0, block // 64)
        def _(i):
            at = pl.ds(pl.multiple_of(s * block + i * 64, 64), 64)
            total = held[e, h, at, :].astype(jnp.float32)
            total = total + from_sib[e // 2, h, at, :].astype(jnp.float32)
            for other in more:
                total = total + other[at, :].astype(jnp.float32)
            if e:
                held[e, h, at, :] = total.astype(jnp.bfloat16)
            else:
                out_ref[at, h * half : (h + 1) * half] = total.astype(jnp.bfloat16)

    def far(s):
        term(s, 7, 0)
        term(s, 6, 0)
        term(s, 7, 1)
        summed(s, 6, 0)
        scatter[s]["six", 0].start()
        term(s, 6, 1)
        term(s, 3, 0)
        summed(s, 6, 1)
        scatter[s]["six", 1].start()
        term(s, 2, 0)
        term(s, 5, 1)
        summed(s, 2, 0)
        scatter[s]["x", 0].start()
        term(s, 4, 1)
        term(s, 3, 1)
        summed(s, 4, 1)
        scatter[s]["y", 1].start()

    def near(s):
        term(s, 2, 1)
        term(s, 5, 0)
        term(s, 4, 0)
        scatter[s]["six", 0].wait_recv()
        summed(s, 4, 0, (from_six.at[0],))
        scatter[s]["y", 0].start()
        scatter[s]["six", 1].wait_recv()
        summed(s, 2, 1, (from_six.at[1],))
        scatter[s]["x", 1].start()

    def last(s):
        for h in range(2):
            scatter[s]["x", h].wait_recv()
            scatter[s]["y", h].wait_recv()
            summed(s, 0, h, (from_x.at[h], from_y.at[h]))

    far(0)
    attend(1, [[(owner, block, block, False)] for owner in others], 4, finish=True)
    near(0)
    far(1)
    for s in range(2):
        for h in range(2):
            term(s, 1, h)
            term(s, 0, h)
    near(1)
    last(0)
    last(1)
    for p in range(3):
        for k in range(3):
            for which in range(2):
                exchange(p, k, which).wait_send()
    for s in range(2):
        for copy in scatter[s].values():
            copy.wait_send()


def rotary_tables(block, count):
    lanes = np.arange(HEAD_DIM)
    rates = rope_base ** (-2.0 * (lanes // 2) / HEAD_DIM)
    sign = np.where(lanes % 2 == 0, -1.0, 1.0)
    inside = np.arange(block)[:, None] * rates[None, :]
    turns = np.stack([np.cos(inside), np.sin(inside)]).astype(np.float32)
    begin = (np.arange(count) * block)[:, None] * rates[None, :]
    cosine, sine = np.cos(begin), np.sin(begin)
    starts = np.stack([cosine, sine, sign * cosine, sign * sine], axis=1)
    starts = np.concatenate([starts, np.zeros_like(starts)], axis=1).astype(np.float32)
    return jnp.asarray(turns), jnp.asarray(starts)


def fused_shards(
    n_cp, n_tp, checkpoint, norm_gain, query_weight, key_weight, value_weight, output_weight, block_order
):
    rows, depth = checkpoint.shape
    q_cols = query_weight.shape[1]
    k_cols = key_weight.shape[1]
    heads = q_cols // HEAD_DIM
    block = rows // 2
    half = depth // 2
    bf16, f32 = jnp.bfloat16, jnp.float32
    turns, starts = rotary_tables(block, block_order.shape[0])
    any_spec = pl.BlockSpec(memory_space=pl.ANY)
    vmem = pl.BlockSpec(memory_space=pltpu.VMEM)
    smem = pl.BlockSpec(memory_space=pltpu.SMEM)
    dma = pltpu.SemaphoreType.DMA
    return pl.pallas_call(
        layer_kernel,
        out_shape=(
            jax.ShapeDtypeStruct((rows, depth), bf16),
            jax.ShapeDtypeStruct((heads, rows), f32),
        ),
        in_specs=[smem] + [any_spec] * 8,
        out_specs=(vmem, vmem),
        scratch_shapes=[
            pltpu.VMEM((8, 2, rows, half), bf16),
            pltpu.VMEM((8, depth, q_cols + 2 * k_cols), bf16),
            pltpu.VMEM((8, 2, q_cols, half), bf16),
            pltpu.VMEM((8, 2, 1, half), f32),
            pltpu.VMEM((rows, q_cols + 2 * k_cols), f32),
            pltpu.VMEM((block, half), bf16),
            pltpu.VMEM((rows, 1), f32),
            pltpu.VMEM((2, block, HEAD_DIM), f32),
            pltpu.VMEM(starts.shape, f32),
            pltpu.VMEM((rows, q_cols), bf16),
            pltpu.VMEM((n_cp, rows, HEAD_DIM), bf16),
            pltpu.VMEM((n_cp, HEAD_DIM + 16, rows), bf16),
            pltpu.VMEM((2 * heads, HEAD_DIM + 16, block), f32),
            pltpu.VMEM((2 * heads, 1, block), f32),
            pltpu.VMEM((4, 2, rows, half), bf16),
            pltpu.VMEM((2, rows, half), bf16),
            pltpu.VMEM((2, rows, half), bf16),
            pltpu.VMEM((2, rows, half), bf16),
            dma((2, 2)),
            dma((8, 3)),
            dma((8, 2)),
            dma((3,)),
            dma((3, 14)),
            dma((3, 14)),
            dma((3, n_cp - 1, 2)),
            dma((3, n_cp, 2)),
            dma((2, 14)),
            dma((2, 14)),
        ],
        compiler_params=pltpu.CompilerParams(
            collective_id=0, has_side_effects=True, vmem_limit_bytes=FUSED_BYTES
        ),
        name="layer",
    )(
        block_order, checkpoint, norm_gain.reshape(8, 2, 1, half), query_weight, key_weight,
        value_weight, output_weight, turns, starts,
    )


def shards(
    n_cp, n_tp, checkpoint, norm_gain, query_weight, key_weight, value_weight, output_weight, block_order
):
    rows = checkpoint.shape[0]
    q_cols = query_weight.shape[1]
    heads = q_cols // HEAD_DIM
    block = rows // 2
    context_rank = lax.axis_index("cp")
    own_blocks = lax.dynamic_slice_in_dim(block_order, 2 * context_rank, 2)
    offsets = jnp.arange(block, dtype=jnp.int32)
    positions = (own_blocks[:, None] * block + offsets[None, :]).reshape(rows)

    vmem = pl.BlockSpec(memory_space=pltpu.VMEM)
    smem = pl.BlockSpec(memory_space=pltpu.SMEM)
    bf16, f32 = jnp.bfloat16, jnp.float32
    dma = pltpu.SemaphoreType.DMA
    queries, key_value = project_any(
        checkpoint, norm_gain, query_weight, key_weight, value_weight, positions
    )
    attended, normalizer = pl.pallas_call(
        functools.partial(attend_kernel, n_cp),
        out_shape=(
            jax.ShapeDtypeStruct((rows, q_cols), bf16),
            jax.ShapeDtypeStruct((heads, rows), f32),
        ),
        in_specs=[smem, vmem, pl.BlockSpec(memory_space=pl.ANY)],
        out_specs=(vmem, vmem),
        scratch_shapes=[
            pltpu.VMEM((n_cp, rows, 2 * HEAD_DIM), bf16),
            pltpu.VMEM((rows, 2 * HEAD_DIM), bf16),
            pltpu.VMEM((rows, rows), f32),
            pltpu.VMEM((heads, rows, 1), f32),
            pltpu.VMEM((heads, rows, 2 * HEAD_DIM), f32),
            pltpu.VMEM((rows, HEAD_DIM), f32),
            dma,
            dma((n_cp - 1, 2)),
            dma((n_cp - 1, 2)),
        ],
        compiler_params=pltpu.CompilerParams(
            collective_id=1, has_side_effects=True, vmem_limit_bytes=VMEM_BYTES
        ),
        name="attend",
    )(block_order, queries, key_value)
    partial_terms = jnp.dot(attended, output_weight, preferred_element_type=jnp.float32)
    projected = lax.psum_scatter(partial_terms.astype(bf16), "tp", scatter_dimension=1, tiled=True)
    return (projected, normalizer)


def solution(mesh):
    n_cp, n_tp = mesh.shape["cp"], mesh.shape["tp"]
    body = fused_shards if (n_cp, n_tp) == (4, 8) else shards
    return jax.shard_map(
        functools.partial(body, n_cp, n_tp),
        mesh=mesh,
        in_specs=(
            P("cp", "tp"),
            P(),
            P(None, "tp"),
            P(None, "tp"),
            P(None, "tp"),
            P("tp", None),
            P(),
        ),
        out_specs=(P("cp", "tp"), P("tp", "cp")),
        check_vma=False,
    )
```

```python
import functools
import math

import jax
import jax.numpy as jnp
import numpy as np
from jax import lax
from jax.experimental import pallas as pl
from jax.experimental.pallas import tpu as pltpu
from jax.sharding import PartitionSpec as P

HEAD_DIM = 128
KV_HEADS = 8
MESH = pl.DeviceIdType.MESH
VMEM_BYTES = 62 * 1024 * 1024
FUSED_BYTES = 64_000_000

rope_base = 500000.0
norm_epsilon = 1e-05
masked_score = -1e30
LOG2E = 1.4426950408889634


def partner_2(block, axis, stride):
    count = lax.axis_size(axis)
    route = []
    for low in range(count):
        high = low | 1 << stride
        if high != low and high < count:
            route += [(low, high), (high, low)]
    return lax.ppermute(block, axis, route)


def turn_pairs(matrix, positions, first_pair):
    pair_count = matrix.shape[-1] // 2
    pair_index = (first_pair + jnp.arange(pair_count, dtype=jnp.int32)).astype(jnp.float32)
    inverse_rates = rope_base ** (-2.0 * pair_index / HEAD_DIM)
    angles = positions.astype(jnp.float32)[:, None] * inverse_rates[None, :]
    cosine = jnp.cos(angles)[:, None, :]
    sine_part = jnp.sin(angles)[:, None, :]
    paired = matrix.reshape(matrix.shape[0], matrix.shape[1], pair_count, 2)
    former = paired[..., 0]
    latter = paired[..., 1]
    turned = jnp.stack(
        [former * cosine - latter * sine_part, former * sine_part + latter * cosine], axis=-1
    )
    return turned.reshape(matrix.shape)


def project_any(checkpoint, norm_gain, query_weight, key_weight, value_weight, positions):
    rows = checkpoint.shape[0]
    heads = query_weight.shape[1] // HEAD_DIM
    key_columns = key_weight.shape[1]
    gathered = lax.all_gather(checkpoint, "tp", axis=1, tiled=True)
    widened = gathered.astype(jnp.float32)
    mean_square = jnp.mean(widened * widened, axis=-1, keepdims=True)
    normed = (widened * lax.rsqrt(mean_square + norm_epsilon) * norm_gain).astype(jnp.bfloat16)
    query_features = jnp.dot(normed, query_weight, preferred_element_type=jnp.float32)
    key_features = jnp.dot(normed, key_weight, preferred_element_type=jnp.float32)
    value_features = jnp.dot(normed, value_weight, preferred_element_type=jnp.float32)
    turned = turn_pairs(query_features.reshape(rows, heads, HEAD_DIM), positions, 0)
    queries = (turned * (LOG2E / math.sqrt(HEAD_DIM))).astype(jnp.bfloat16)
    sharing = lax.axis_size("tp") // KV_HEADS
    part_of_head = lax.axis_index("tp") % sharing
    key_part = turn_pairs(
        key_features.reshape(rows, 1, key_columns), positions, part_of_head * (key_columns // 2)
    )
    key_part = key_part.astype(jnp.bfloat16).reshape(rows, key_columns)
    own_pair = jnp.stack([key_part, value_features.astype(jnp.bfloat16)])
    key_value = own_pair
    if sharing == 2:
        partner = partner_2(own_pair, "tp", 0)
        lower_first = jnp.concatenate([own_pair, partner], axis=-1)
        upper_first = jnp.concatenate([partner, own_pair], axis=-1)
        key_value = jnp.where(part_of_head == 0, lower_first, upper_first)
    return (
        queries.reshape(rows, heads * HEAD_DIM),
        jnp.concatenate([key_value[0], key_value[1]], axis=-1),
    )


def flipped(me, offset):
    result = me
    for bit in (1, 2, 4):
        chosen = offset // bit % 2
        result = result + chosen * (bit - 2 * bit * (me // bit % 2))
    return result


def greet(axis, others):
    barrier = pltpu.get_barrier_semaphore()
    for other in others:
        pl.semaphore_signal(barrier, inc=1, device_id={axis: other}, device_id_type=MESH)
    pl.semaphore_wait(barrier, len(others))


def attend_kernel(
    n_cp, order_ref, q_ref, kv_hbm, out_ref, norm_ref,
    ring, extended, bias, top, weighted, norms, kv_sem, send_sems, recv_sems,
):
    me = lax.axis_index("cp")
    rows = q_ref.shape[0]
    block = rows // 2
    heads = q_ref.shape[1] // HEAD_DIM
    right, left = lax.rem(me + 1, n_cp), lax.rem(me + n_cp - 1, n_cp)
    own_copy = pltpu.make_async_copy(kv_hbm, ring.at[0], kv_sem)
    own_copy.start()
    greet("cp", (right, left))
    own_copy.wait()

    def hop(step, h):
        at = pl.ds(h * block, block)
        return pltpu.make_async_remote_copy(
            src_ref=ring.at[step, at, :],
            dst_ref=ring.at[step + 1, at, :],
            send_sem=send_sems.at[step, h],
            recv_sem=recv_sems.at[step, h],
            device_id={"cp": right},
            device_id_type=MESH,
        )

    hop(0, 0).start()
    hop(0, 1).start()
    extended[:, HEAD_DIM:] = jnp.ones((rows, HEAD_DIM), jnp.bfloat16)
    top[...] = jnp.full(top.shape, masked_score, jnp.float32)
    weighted[...] = jnp.zeros_like(weighted)

    def visit(step, carried):
        for h in range(2):

            @pl.when(step > 0)
            def _():
                hop(step - 1, h).wait_recv()

            @pl.when(jnp.logical_and(step > 0, step < n_cp - 1))
            def _():
                hop(step, h).start()

        owner = lax.rem(me - step + n_cp, n_cp)
        extended[:, :HEAD_DIM] = ring[step, :, HEAD_DIM:]
        base = lax.broadcasted_iota(jnp.int32, (block, block), 0) - lax.broadcasted_iota(
            jnp.int32, (block, block), 1
        )
        for i in range(2):
            for j in range(2):
                ahead = (order_ref[2 * me + i] - order_ref[2 * owner + j]) * block
                bias[i * block : (i + 1) * block, j * block : (j + 1) * block] = jnp.where(
                    base + ahead >= 0, 0.0, masked_score
                )

        def one_head(h, inner):
            cols = pl.ds(pl.multiple_of(h * HEAD_DIM, HEAD_DIM), HEAD_DIM)
            keys = ring[step, :, :HEAD_DIM]
            for i in range(2):
                at = pl.ds(i * block, block)
                scores = lax.dot_general(
                    q_ref[at, cols], keys, (((1,), (1,)), ((), ())),
                    preferred_element_type=jnp.float32,
                )
                scores = scores + bias[at, :]
                old_top = top[h, at, :]
                new_top = jnp.maximum(old_top, jnp.max(scores, axis=1, keepdims=True))
                weights = jnp.exp2(scores - new_top).astype(jnp.bfloat16)
                shrink = jnp.exp2(old_top - new_top)
                top[h, at, :] = new_top
                weighted[h, at, :] = weighted[h, at, :] * shrink + jnp.dot(
                    weights, extended[...], preferred_element_type=jnp.float32
                )
            return inner

        lax.fori_loop(0, heads, one_head, 0, unroll=2)
        return carried

    lax.fori_loop(0, n_cp, visit, 0)
    lane = lax.broadcasted_iota(jnp.int32, (rows, HEAD_DIM), 1)
    norms[...] = jnp.zeros_like(norms)
    for h in range(heads):
        totals = weighted[h, :, HEAD_DIM:]
        out_ref[:, h * HEAD_DIM : (h + 1) * HEAD_DIM] = (
            weighted[h, :, :HEAD_DIM] / totals
        ).astype(jnp.bfloat16)
        norm = (top[h] + jnp.log2(totals)) * (1.0 / LOG2E)
        norms[...] = jnp.where(lane == h, norm, norms[...])
    norm_ref[...] = jnp.transpose(norms[...])[:heads, :]

    for step in range(n_cp - 1):
        for h in range(2):
            hop(step, h).wait_send()


def layer_kernel(
    order_hbm, x_hbm, gain_hbm, wq_hbm, wk_hbm, wv_hbm, wo_hbm, turns_hbm, starts_hbm,
    out_ref, norm_ref,
    order_ref, held, weights, out_weights, gains, acc, squares, turns, starts,
    queries, keys, values, weighted, top, from_sib, from_six, from_x, from_y,
    x_sems, w_sems, o_sems, t_sems, ag_send, ag_recv, kv_send, kv_recv, rs_send, rs_recv,
):
    me = lax.axis_index("tp")
    z = lax.axis_index("cp")
    rows, depth = x_hbm.shape
    half = depth // 2
    block = rows // 2
    q_cols = wq_hbm.shape[1]
    k_cols = wk_hbm.shape[1]
    heads = q_cols // HEAD_DIM
    kv_end = q_cols + 2 * k_cols
    sib, nx, ny = flipped(me, 1), flipped(me, 2), flipped(me, 4)
    pieces = ((0, block), (block, block // 2), (block + block // 2, block // 2))

    upper = z // 2
    low = z + upper * (3 - 2 * z)
    others = []
    for k in range(3):
        near = k + 1 - (low if k == 0 else 0)
        others.append(near + upper * (3 - 2 * near))

    x_copies = []
    for p, (first, count) in enumerate(((0, block), (block, block))):
        for h in range(2):
            at = pl.ds(first, count)
            x_copies.append(
                pltpu.make_async_copy(
                    x_hbm.at[at, pl.ds(h * half, half)], held.at[0, h, at, :], x_sems.at[p, h]
                )
            )
    for copy in x_copies:
        copy.start()
    small = [
        pltpu.make_async_copy(gain_hbm, gains, t_sems.at[0]),
        pltpu.make_async_copy(turns_hbm, turns, t_sems.at[1]),
        pltpu.make_async_copy(starts_hbm, starts, t_sems.at[2]),
        pltpu.make_async_copy(order_hbm, order_ref, t_sems.at[3]),
    ]
    small[0].start()
    small[3].start()
    w_copies = []
    for e in range(8):
        chunk = pl.ds(pl.multiple_of(flipped(me, e) * depth, depth), depth)
        parts = ((wq_hbm, 0, q_cols), (wk_hbm, q_cols, k_cols), (wv_hbm, q_cols + k_cols, k_cols))
        w_copies.append(
            [
                pltpu.make_async_copy(
                    w.at[chunk, :], weights.at[e, :, pl.ds(at, size)], w_sems.at[e, i]
                )
                for i, (w, at, size) in enumerate(parts)
            ]
        )
    o_copies = {}
    for e in (7, 6, 3, 2, 5, 4, 1, 0):
        for h in range(2):
            at = pl.ds(pl.multiple_of(flipped(me, e) * depth + h * half, half), half)
            o_copies[e, h] = pltpu.make_async_copy(
                wo_hbm.at[:, at], out_weights.at[e, h], o_sems.at[e, h]
            )

    barrier = pltpu.get_barrier_semaphore()
    peers = [{"tp": sib}, {"tp": nx}, {"tp": ny}] + [{"cp": other} for other in others]
    for peer in peers:
        pl.semaphore_signal(barrier, inc=1, device_id=peer, device_id_type=MESH)
    pl.semaphore_wait(barrier, len(peers))

    def remote(source, target, send, recv, device):
        return pltpu.make_async_remote_copy(
            src_ref=source, dst_ref=target, send_sem=send, recv_sem=recv,
            device_id=device, device_id_type=MESH,
        )

    gather = []
    for p, (first, count) in enumerate(pieces):
        at = pl.ds(first, count)

        def part(slot, h, at=at):
            return held.at[slot, h, at, :]

        plan = {
            "dx0": (0, 0, 2, nx), "dx1": (0, 1, 2, nx), "dy0": (0, 0, 4, ny), "dy1": (0, 1, 4, ny),
            "s0": (0, 0, 1, sib), "s1": (0, 1, 1, sib), "fy": (2, 0, 6, ny), "fx": (4, 1, 6, nx),
            "a0": (2, 0, 3, sib), "a1": (2, 1, 3, sib), "b0": (4, 0, 5, sib), "b1": (4, 1, 5, sib),
            "c0": (6, 0, 7, sib), "c1": (6, 1, 7, sib),
        }
        gather.append(
            {
                name: remote(
                    part(slot, h), part(to, h), ag_send.at[p, i], ag_recv.at[p, i], {"tp": other}
                )
                for i, (name, (slot, h, to, other)) in enumerate(plan.items())
            }
        )

    def send(p, *names):
        for name in names:
            gather[p][name].start()

    def landed(p, *names):
        for name in names:
            gather[p][name].wait_recv()

    for copy in x_copies[:2]:
        copy.wait()
    send(0, "dx0", "dy1", "dx1", "dy0", "s0", "s1")
    for copies in w_copies:
        for copy in copies:
            copy.start()
    small[1].start()
    small[2].start()
    acc[...] = jnp.zeros_like(acc)
    squares[...] = jnp.zeros_like(squares)
    values[:, HEAD_DIM:, :] = jnp.ones((4, 16, rows), jnp.bfloat16)
    for copy in x_copies[2:]:
        copy.wait()
    for p in (1, 2):
        send(p, "s0", "s1")
    small[0].wait()

    def weights_of(*slots):
        for e in slots:
            for copy in w_copies[e]:
                copy.wait()

    def process(first, count, chunks, chunk_of, low=0, high=kv_end):
        at = pl.ds(first, count)

        @pl.loop(0, chunks)
        def _(i):
            e, h = chunk_of(i)
            wide = held[e, h, at, :].astype(jnp.float32)
            if high == kv_end:
                squares[at, :] += jnp.sum(wide * wide, axis=1, keepdims=True)
            acc[at, low:high] += jnp.dot(
                (wide * gains[flipped(me, e), h]).astype(jnp.bfloat16),
                weights[e, pl.ds(pl.multiple_of(h * half, half), half), low:high],
                preferred_element_type=jnp.float32,
            )

    def own_pair(i):
        return i // 2, i % 2

    def early(i):
        return 2 + i, i // 2

    def late(i):
        return 2 + i, 1 - i // 2

    score_scale = LOG2E / math.sqrt(HEAD_DIM)
    features = depth * 8

    def exchange(p, k, which):
        first, count = pieces[p]
        if which == 0:
            ref = keys.at[z, pl.ds(first, count), :]
        else:
            ref = values.at[z, pl.ds(0, HEAD_DIM), pl.ds(first, count)]
        return remote(ref, ref, kv_send.at[p, k, which], kv_recv.at[p, z, which], {"cp": others[k]})

    def arrived(p, owner):
        first, count = pieces[p]
        refs = (
            keys.at[owner, pl.ds(first, count), :],
            values.at[owner, pl.ds(0, HEAD_DIM), pl.ds(first, count)],
        )
        for which, ref in enumerate(refs):
            remote(
                ref, ref, kv_send.at[p, 0, which], kv_recv.at[p, owner, which], {"cp": others[0]}
            ).wait_recv()

    def turner(first, j, sub):
        start = starts[order_ref[2 * z + first // block]]
        at = pl.ds(pl.multiple_of(first % block + j * sub, sub), sub)
        cosine = turns[0, at, :] * start[0:1, :] - turns[1, at, :] * start[1:2, :]
        sine = turns[1, at, :] * start[2:3, :] + turns[0, at, :] * start[3:4, :]
        even = lax.rem(lax.broadcasted_iota(jnp.int32, (sub, HEAD_DIM), 1), 2) == 0

        def turned(content):
            later = pltpu.roll(content, HEAD_DIM - 1, 1)
            former = pltpu.roll(content, 1, 1)
            return content * cosine + jnp.where(even, later, former) * sine

        return turned

    def rate_of(at):
        return lax.rsqrt(squares[at, :] * (1.0 / features) + norm_epsilon)

    def finish_keys(p):
        first, count = pieces[p]

        @pl.loop(0, count // 128)
        def _(j):
            at = pl.ds(pl.multiple_of(first + j * 128, 128), 128)
            rate = rate_of(at)
            turned = turner(first, j, 128)
            keys[z, at, :] = turned(acc[at, q_cols : q_cols + k_cols] * rate).astype(jnp.bfloat16)
            value = acc[at, q_cols + k_cols : kv_end] * rate
            values[z, :HEAD_DIM, at] = jnp.transpose(value).astype(jnp.bfloat16)

        for k in (2, 1, 0):
            for which in (0, 1):
                exchange(p, k, which).start()

    def finish_queries(p):
        first, count = pieces[p]

        @pl.loop(0, count // 64)
        def _(j):
            at = pl.ds(pl.multiple_of(first + j * 64, 64), 64)
            rate = rate_of(at) * score_scale
            turned = turner(first, j, 64)
            for h in range(heads):
                cols = pl.ds(h * HEAD_DIM, HEAD_DIM)
                queries[at, cols] = turned(acc[at, cols] * rate).astype(jnp.bfloat16)

    def visible(s, owner, j):
        ahead = order_ref[2 * z + s] - order_ref[2 * owner + j]
        return jnp.where(ahead > 0, 0.0, masked_score)

    def attend(s, chunks, together, start=False, finish=False):
        q_at = pl.ds(s * block, block)
        shades = {}
        for chunk in chunks:
            for owner, first, count, diagonal in chunk:
                if not diagonal:
                    shades[id(owner), first] = visible(s, owner, first // block)

        def columns(h):
            return pl.ds(pl.multiple_of(h * HEAD_DIM, HEAD_DIM), HEAD_DIM)

        def place(side, j, offset, count):
            return pl.ds(side * block + offset, count), pl.ds(j * block, block)

        def scored(h, side, j, peak):
            offset = 0
            for owner, first, count, diagonal in chunks[j]:
                scores = lax.dot_general(
                    keys[owner, pl.ds(first, count), :], queries[q_at, columns(h)],
                    (((1,), (1,)), ((), ())), preferred_element_type=jnp.float32,
                )
                if diagonal:
                    key_at = lax.broadcasted_iota(jnp.int32, (count, block), 0)
                    query_at = lax.broadcasted_iota(jnp.int32, (count, block), 1)
                    scores = jnp.where(key_at <= query_at, scores, masked_score)
                acc[place(side, j, offset, count)] = scores
                offset += count
                highest = jnp.max(scores, axis=0, keepdims=True)
                if not diagonal:
                    highest = highest + shades[id(owner), first]
                peak = highest if peak is None else jnp.maximum(peak, highest)
            return peak

        def beside(coming, side, h, peak):
            slot = s * heads + h
            new_top = peak
            if not start:
                old_top = top[slot]
                new_top = jnp.maximum(old_top, peak)
                shrink = jnp.exp2(old_top - new_top)
            next_peak, total = None, None
            for j, chunk in enumerate(chunks):
                if coming is not None:
                    next_peak = scored(coming, 1 - side, j, next_peak)
                offset = 0
                shares, extended = [], []
                for owner, first, count, diagonal in chunk:
                    lean = new_top if diagonal else new_top - shades[id(owner), first]
                    scores = acc[place(side, j, offset, count)]
                    shares.append(jnp.exp2(scores - lean).astype(jnp.bfloat16))
                    extended.append(values[owner, :, pl.ds(first, count)])
                    offset += count
                share, wide = shares[0], extended[0]
                if len(chunk) > 1:
                    share, wide = jnp.concatenate(shares, 0), jnp.concatenate(extended, 1)
                piece = jnp.dot(wide, share, preferred_element_type=jnp.float32)
                total = piece if total is None else total + piece
            if not start:
                total = weighted[slot] * shrink + total
            if finish:
                sums = total[HEAD_DIM : HEAD_DIM + 1, :]
                part = total[:HEAD_DIM, :] * (1.0 / sums)
                queries[q_at, columns(h)] = jnp.transpose(part).astype(jnp.bfloat16)
                norm_ref[pl.ds(h, 1), q_at] = (new_top + jnp.log2(sums)) * (1.0 / LOG2E)
            else:
                weighted[slot] = total
                top[slot] = new_top
            return next_peak

        peak = None
        for j in range(len(chunks)):
            peak = scored(0, 0, j, peak)
        if together == heads:
            for h in range(heads):
                peak = beside(h + 1 if h + 1 < heads else None, h % 2, h, peak)
        else:

            def group(i, peak):
                for u in range(together):
                    h = i * together + u
                    coming = h + 1 if u + 1 < together else jnp.minimum(h + 1, heads - 1)
                    peak = beside(coming, u % 2, h, peak)
                return peak

            lax.fori_loop(0, heads // together, group, peak)

    weights_of(0, 1)
    landed(0, "s0", "s1")
    process(*pieces[0], 4, own_pair)
    landed(0, "dx0")
    send(0, "fy", "a0")
    landed(0, "dy1")
    send(0, "fx", "b1")
    send(1, "dx0", "dy1", "dx1", "dy0")
    send(2, "dx0", "dy1")
    for copy in o_copies.values():
        copy.start()
    weights_of(2, 3, 4, 5)
    landed(0, "a0", "b1")
    process(*pieces[0], 4, early)
    landed(0, "dx1")
    send(0, "a1")
    landed(0, "dy0")
    send(0, "b0")
    for p in (1, 2):
        landed(p, "s0", "s1")
    process(block, block, 4, own_pair)
    landed(0, "a1", "b0")
    process(*pieces[0], 4, late)
    weights_of(6, 7)
    landed(0, "fy")
    send(0, "c0")
    landed(0, "fx")
    send(0, "c1")
    process(*pieces[0], 2, lambda i: (6, i))
    landed(0, "c0", "c1")
    process(*pieces[0], 2, lambda i: (7, i))
    for copy in small[1:]:
        copy.wait()
    finish_keys(0)
    landed(1, "dx0")
    send(1, "fy", "a0")
    landed(1, "dy1")
    send(1, "fx", "b1")
    send(2, "dx1", "dy0")
    finish_queries(0)
    landed(1, "a0", "b1")
    process(*pieces[1], 4, early)
    landed(1, "dx1")
    send(1, "a1")
    landed(1, "dy0")
    send(1, "b0")
    landed(1, "a1", "b0")
    process(*pieces[1], 4, late)
    landed(2, "dx0")
    send(2, "fy", "a0")
    landed(2, "dy1")
    send(2, "fx", "b1")
    landed(2, "a0", "b1")
    process(*pieces[2], 4, early)
    landed(1, "fy")
    send(1, "c0")
    landed(1, "fx")
    send(1, "c1")
    process(*pieces[1], 2, lambda i: (6, i))
    landed(1, "c0", "c1")
    process(*pieces[1], 2, lambda i: (7, i))
    finish_keys(1)
    finish_queries(1)
    third = block // 2
    near, middle, distant = others
    landed(2, "dx1")
    send(2, "a1")
    landed(2, "dy0")
    send(2, "b0")
    landed(2, "a1", "b0")
    process(*pieces[2], 4, late)
    landed(2, "fy")
    send(2, "c0")
    landed(2, "fx")
    send(2, "c1")
    process(*pieces[2], 2, lambda i: (6, i), q_cols)
    landed(2, "c0", "c1")
    process(*pieces[2], 2, lambda i: (7, i), q_cols)
    finish_keys(2)
    process(*pieces[2], 4, lambda i: (6 + i // 2, i % 2), 0, q_cols)
    finish_queries(2)

    for owner in others:
        arrived(0, owner)
    whole = [[(owner, 0, block, False)] for owner in others]
    attend(0, [[(z, 0, block, True)], [(z, block, block, False)]] + whole, 4, start=True)
    for owner in others:
        arrived(1, owner)
    attend(
        0,
        [
            [(near, block, third, False), (middle, block, third, False)],
            [(distant, block, third, False)],
        ],
        4,
    )
    for p in range(3):
        for copy in gather[p].values():
            copy.wait_send()
    for owner in others:
        arrived(2, owner)
    attend(
        0,
        [
            [(near, block + third, third, False), (middle, block + third, third, False)],
            [(distant, block + third, third, False)],
        ],
        heads,
        finish=True,
    )

    scatter = []
    for s in range(2):
        at = pl.ds(s * block, block)
        plan = {}
        for e in (1, 3, 5, 7):
            for h in range(2):
                plan["s", e, h] = (held.at[e, h, at, :], from_sib.at[e // 2, h, at, :], sib)
        plan["six", 0] = (held.at[6, 0, at, :], from_six.at[0, at, :], nx)
        plan["six", 1] = (held.at[6, 1, at, :], from_six.at[1, at, :], ny)
        for h in range(2):
            plan["x", h] = (held.at[2, h, at, :], from_x.at[h, at, :], nx)
            plan["y", h] = (held.at[4, h, at, :], from_y.at[h, at, :], ny)
        scatter.append(
            {
                name: remote(source, target, rs_send.at[s, i], rs_recv.at[s, i], {"tp": other})
                for i, (name, (source, target, other)) in enumerate(plan.items())
            }
        )

    def term(s, e, h):
        if s == 0:
            o_copies[e, h].wait()
        at = pl.ds(s * block, block)
        held[e, h, at, :] = jnp.dot(
            queries[at, :], out_weights[e, h], preferred_element_type=jnp.float32
        ).astype(jnp.bfloat16)
        if e % 2:
            scatter[s]["s", e, h].start()

    def summed(s, e, h, more=()):
        scatter[s]["s", e + 1, h].wait_recv()

        @pl.loop(0, block // 64)
        def _(i):
            at = pl.ds(pl.multiple_of(s * block + i * 64, 64), 64)
            total = held[e, h, at, :].astype(jnp.float32)
            total = total + from_sib[e // 2, h, at, :].astype(jnp.float32)
            for other in more:
                total = total + other[at, :].astype(jnp.float32)
            if e:
                held[e, h, at, :] = total.astype(jnp.bfloat16)
            else:
                out_ref[at, h * half : (h + 1) * half] = total.astype(jnp.bfloat16)

    def far(s):
        term(s, 7, 0)
        term(s, 6, 0)
        term(s, 7, 1)
        summed(s, 6, 0)
        scatter[s]["six", 0].start()
        term(s, 6, 1)
        term(s, 3, 0)
        summed(s, 6, 1)
        scatter[s]["six", 1].start()
        term(s, 2, 0)
        term(s, 5, 1)
        summed(s, 2, 0)
        scatter[s]["x", 0].start()
        term(s, 4, 1)
        term(s, 3, 1)
        summed(s, 4, 1)
        scatter[s]["y", 1].start()

    def near(s):
        term(s, 2, 1)
        term(s, 5, 0)
        term(s, 4, 0)
        scatter[s]["six", 0].wait_recv()
        summed(s, 4, 0, (from_six.at[0],))
        scatter[s]["y", 0].start()
        scatter[s]["six", 1].wait_recv()
        summed(s, 2, 1, (from_six.at[1],))
        scatter[s]["x", 1].start()

    def last(s):
        for h in range(2):
            scatter[s]["x", h].wait_recv()
            scatter[s]["y", h].wait_recv()
            summed(s, 0, h, (from_x.at[h], from_y.at[h]))

    far(0)
    attend(1, [[(z, block, block, True)], [(z, 0, block, False)]] + whole, 4, start=True)
    near(0)
    attend(1, [[(owner, block, block, False)] for owner in others], 4, finish=True)
    far(1)
    for s in range(2):
        for h in range(2):
            term(s, 1, h)
            term(s, 0, h)
    near(1)
    last(0)
    last(1)
    for p in range(3):
        for k in range(3):
            for which in range(2):
                exchange(p, k, which).wait_send()
    for s in range(2):
        for copy in scatter[s].values():
            copy.wait_send()


def rotary_tables(block, count):
    lanes = np.arange(HEAD_DIM)
    rates = rope_base ** (-2.0 * (lanes // 2) / HEAD_DIM)
    sign = np.where(lanes % 2 == 0, -1.0, 1.0)
    inside = np.arange(block)[:, None] * rates[None, :]
    turns = np.stack([np.cos(inside), np.sin(inside)]).astype(np.float32)
    begin = (np.arange(count) * block)[:, None] * rates[None, :]
    cosine, sine = np.cos(begin), np.sin(begin)
    starts = np.stack([cosine, sine, sign * cosine, sign * sine], axis=1)
    starts = np.concatenate([starts, np.zeros_like(starts)], axis=1).astype(np.float32)
    return jnp.asarray(turns), jnp.asarray(starts)


def store_kernel(out_ref, norm_ref, out_hbm, norm_hbm, sems):
    copies = [
        pltpu.make_async_copy(out_ref, out_hbm, sems.at[0]),
        pltpu.make_async_copy(norm_ref, norm_hbm, sems.at[1]),
    ]
    for copy in copies:
        copy.start()
    for copy in copies:
        copy.wait()


def fused_shards(
    n_cp, n_tp, checkpoint, norm_gain, query_weight, key_weight, value_weight, output_weight, block_order
):
    rows, depth = checkpoint.shape
    q_cols = query_weight.shape[1]
    k_cols = key_weight.shape[1]
    heads = q_cols // HEAD_DIM
    block = rows // 2
    half = depth // 2
    bf16, f32 = jnp.bfloat16, jnp.float32
    turns, starts = rotary_tables(block, block_order.shape[0])
    any_spec = pl.BlockSpec(memory_space=pl.ANY)
    vmem = pl.BlockSpec(memory_space=pltpu.VMEM)
    dma = pltpu.SemaphoreType.DMA
    results = pl.pallas_call(
        layer_kernel,
        out_shape=(pltpu.VMEM((rows, depth), bf16), pltpu.VMEM((heads, rows), f32)),
        in_specs=[any_spec] * 9,
        out_specs=(vmem, vmem),
        scratch_shapes=[
            pltpu.SMEM(block_order.shape, jnp.int32),
            pltpu.VMEM((8, 2, rows, half), bf16),
            pltpu.VMEM((8, depth, q_cols + 2 * k_cols), bf16),
            pltpu.VMEM((8, 2, q_cols, half), bf16),
            pltpu.VMEM((8, 2, 1, half), f32),
            pltpu.VMEM((rows, q_cols + 2 * k_cols), f32),
            pltpu.VMEM((rows, 1), f32),
            pltpu.VMEM((2, block, HEAD_DIM), f32),
            pltpu.VMEM(starts.shape, f32),
            pltpu.VMEM((rows, q_cols), bf16),
            pltpu.VMEM((n_cp, rows, HEAD_DIM), bf16),
            pltpu.VMEM((n_cp, HEAD_DIM + 16, rows), bf16),
            pltpu.VMEM((2 * heads, HEAD_DIM + 16, block), f32),
            pltpu.VMEM((2 * heads, 1, block), f32),
            pltpu.VMEM((4, 2, rows, half), bf16),
            pltpu.VMEM((2, rows, half), bf16),
            pltpu.VMEM((2, rows, half), bf16),
            pltpu.VMEM((2, rows, half), bf16),
            dma((2, 2)),
            dma((8, 3)),
            dma((8, 2)),
            dma((4,)),
            dma((3, 14)),
            dma((3, 14)),
            dma((3, n_cp - 1, 2)),
            dma((3, n_cp, 2)),
            dma((2, 14)),
            dma((2, 14)),
        ],
        compiler_params=pltpu.CompilerParams(
            collective_id=0, has_side_effects=True, vmem_limit_bytes=FUSED_BYTES
        ),
        name="layer",
    )(
        block_order, checkpoint, norm_gain.reshape(8, 2, 1, half), query_weight, key_weight,
        value_weight, output_weight, turns, starts,
    )
    return pl.pallas_call(
        store_kernel,
        out_shape=(
            jax.ShapeDtypeStruct((rows, depth), bf16),
            jax.ShapeDtypeStruct((heads, rows), f32),
        ),
        in_specs=[vmem, vmem],
        out_specs=(any_spec, any_spec),
        scratch_shapes=[dma((2,))],
        compiler_params=pltpu.CompilerParams(vmem_limit_bytes=1 << 20),
        name="store",
    )(*results)


def shards(
    n_cp, n_tp, checkpoint, norm_gain, query_weight, key_weight, value_weight, output_weight, block_order
):
    rows = checkpoint.shape[0]
    q_cols = query_weight.shape[1]
    heads = q_cols // HEAD_DIM
    block = rows // 2
    context_rank = lax.axis_index("cp")
    own_blocks = lax.dynamic_slice_in_dim(block_order, 2 * context_rank, 2)
    offsets = jnp.arange(block, dtype=jnp.int32)
    positions = (own_blocks[:, None] * block + offsets[None, :]).reshape(rows)

    vmem = pl.BlockSpec(memory_space=pltpu.VMEM)
    smem = pl.BlockSpec(memory_space=pltpu.SMEM)
    bf16, f32 = jnp.bfloat16, jnp.float32
    dma = pltpu.SemaphoreType.DMA
    queries, key_value = project_any(
        checkpoint, norm_gain, query_weight, key_weight, value_weight, positions
    )
    attended, normalizer = pl.pallas_call(
        functools.partial(attend_kernel, n_cp),
        out_shape=(
            jax.ShapeDtypeStruct((rows, q_cols), bf16),
            jax.ShapeDtypeStruct((heads, rows), f32),
        ),
        in_specs=[smem, vmem, pl.BlockSpec(memory_space=pl.ANY)],
        out_specs=(vmem, vmem),
        scratch_shapes=[
            pltpu.VMEM((n_cp, rows, 2 * HEAD_DIM), bf16),
            pltpu.VMEM((rows, 2 * HEAD_DIM), bf16),
            pltpu.VMEM((rows, rows), f32),
            pltpu.VMEM((heads, rows, 1), f32),
            pltpu.VMEM((heads, rows, 2 * HEAD_DIM), f32),
            pltpu.VMEM((rows, HEAD_DIM), f32),
            dma,
            dma((n_cp - 1, 2)),
            dma((n_cp - 1, 2)),
        ],
        compiler_params=pltpu.CompilerParams(
            collective_id=1, has_side_effects=True, vmem_limit_bytes=VMEM_BYTES
        ),
        name="attend",
    )(block_order, queries, key_value)
    partial_terms = jnp.dot(attended, output_weight, preferred_element_type=jnp.float32)
    projected = lax.psum_scatter(partial_terms.astype(bf16), "tp", scatter_dimension=1, tiled=True)
    return (projected, normalizer)


def solution(mesh):
    n_cp, n_tp = mesh.shape["cp"], mesh.shape["tp"]
    body = fused_shards if (n_cp, n_tp) == (4, 8) else shards
    return jax.shard_map(
        functools.partial(body, n_cp, n_tp),
        mesh=mesh,
        in_specs=(
            P("cp", "tp"),
            P(),
            P(None, "tp"),
            P(None, "tp"),
            P(None, "tp"),
            P("tp", None),
            P(),
        ),
        out_specs=(P("cp", "tp"), P("tp", "cp")),
        check_vma=False,
    )
```

```python
import functools
import math

import jax
import jax.numpy as jnp
import numpy as np
from jax import lax
from jax.experimental import pallas as pl
from jax.experimental.pallas import tpu as pltpu
from jax.sharding import PartitionSpec as P

HEAD_DIM = 128
KV_HEADS = 8
MESH = pl.DeviceIdType.MESH
VMEM_BYTES = 62 * 1024 * 1024
FUSED_BYTES = 64_000_000

rope_base = 500000.0
norm_epsilon = 1e-05
masked_score = -1e30
LOG2E = 1.4426950408889634


def partner_2(block, axis, stride):
    count = lax.axis_size(axis)
    route = []
    for low in range(count):
        high = low | 1 << stride
        if high != low and high < count:
            route += [(low, high), (high, low)]
    return lax.ppermute(block, axis, route)


def turn_pairs(matrix, positions, first_pair):
    pair_count = matrix.shape[-1] // 2
    pair_index = (first_pair + jnp.arange(pair_count, dtype=jnp.int32)).astype(jnp.float32)
    inverse_rates = rope_base ** (-2.0 * pair_index / HEAD_DIM)
    angles = positions.astype(jnp.float32)[:, None] * inverse_rates[None, :]
    cosine = jnp.cos(angles)[:, None, :]
    sine_part = jnp.sin(angles)[:, None, :]
    paired = matrix.reshape(matrix.shape[0], matrix.shape[1], pair_count, 2)
    former = paired[..., 0]
    latter = paired[..., 1]
    turned = jnp.stack(
        [former * cosine - latter * sine_part, former * sine_part + latter * cosine], axis=-1
    )
    return turned.reshape(matrix.shape)


def project_any(checkpoint, norm_gain, query_weight, key_weight, value_weight, positions):
    rows = checkpoint.shape[0]
    heads = query_weight.shape[1] // HEAD_DIM
    key_columns = key_weight.shape[1]
    gathered = lax.all_gather(checkpoint, "tp", axis=1, tiled=True)
    widened = gathered.astype(jnp.float32)
    mean_square = jnp.mean(widened * widened, axis=-1, keepdims=True)
    normed = (widened * lax.rsqrt(mean_square + norm_epsilon) * norm_gain).astype(jnp.bfloat16)
    query_features = jnp.dot(normed, query_weight, preferred_element_type=jnp.float32)
    key_features = jnp.dot(normed, key_weight, preferred_element_type=jnp.float32)
    value_features = jnp.dot(normed, value_weight, preferred_element_type=jnp.float32)
    turned = turn_pairs(query_features.reshape(rows, heads, HEAD_DIM), positions, 0)
    queries = (turned * (LOG2E / math.sqrt(HEAD_DIM))).astype(jnp.bfloat16)
    sharing = lax.axis_size("tp") // KV_HEADS
    part_of_head = lax.axis_index("tp") % sharing
    key_part = turn_pairs(
        key_features.reshape(rows, 1, key_columns), positions, part_of_head * (key_columns // 2)
    )
    key_part = key_part.astype(jnp.bfloat16).reshape(rows, key_columns)
    own_pair = jnp.stack([key_part, value_features.astype(jnp.bfloat16)])
    key_value = own_pair
    if sharing == 2:
        partner = partner_2(own_pair, "tp", 0)
        lower_first = jnp.concatenate([own_pair, partner], axis=-1)
        upper_first = jnp.concatenate([partner, own_pair], axis=-1)
        key_value = jnp.where(part_of_head == 0, lower_first, upper_first)
    return (
        queries.reshape(rows, heads * HEAD_DIM),
        jnp.concatenate([key_value[0], key_value[1]], axis=-1),
    )


def flipped(me, offset):
    result = me
    for bit in (1, 2, 4):
        chosen = offset // bit % 2
        result = result + chosen * (bit - 2 * bit * (me // bit % 2))
    return result


def greet(axis, others):
    barrier = pltpu.get_barrier_semaphore()
    for other in others:
        pl.semaphore_signal(barrier, inc=1, device_id={axis: other}, device_id_type=MESH)
    pl.semaphore_wait(barrier, len(others))


def attend_kernel(
    n_cp, order_ref, q_ref, kv_hbm, out_ref, norm_ref,
    ring, extended, bias, top, weighted, norms, kv_sem, send_sems, recv_sems,
):
    me = lax.axis_index("cp")
    rows = q_ref.shape[0]
    block = rows // 2
    heads = q_ref.shape[1] // HEAD_DIM
    right, left = lax.rem(me + 1, n_cp), lax.rem(me + n_cp - 1, n_cp)
    own_copy = pltpu.make_async_copy(kv_hbm, ring.at[0], kv_sem)
    own_copy.start()
    greet("cp", (right, left))
    own_copy.wait()

    def hop(step, h):
        at = pl.ds(h * block, block)
        return pltpu.make_async_remote_copy(
            src_ref=ring.at[step, at, :],
            dst_ref=ring.at[step + 1, at, :],
            send_sem=send_sems.at[step, h],
            recv_sem=recv_sems.at[step, h],
            device_id={"cp": right},
            device_id_type=MESH,
        )

    hop(0, 0).start()
    hop(0, 1).start()
    extended[:, HEAD_DIM:] = jnp.ones((rows, HEAD_DIM), jnp.bfloat16)
    top[...] = jnp.full(top.shape, masked_score, jnp.float32)
    weighted[...] = jnp.zeros_like(weighted)

    def visit(step, carried):
        for h in range(2):

            @pl.when(step > 0)
            def _():
                hop(step - 1, h).wait_recv()

            @pl.when(jnp.logical_and(step > 0, step < n_cp - 1))
            def _():
                hop(step, h).start()

        owner = lax.rem(me - step + n_cp, n_cp)
        extended[:, :HEAD_DIM] = ring[step, :, HEAD_DIM:]
        base = lax.broadcasted_iota(jnp.int32, (block, block), 0) - lax.broadcasted_iota(
            jnp.int32, (block, block), 1
        )
        for i in range(2):
            for j in range(2):
                ahead = (order_ref[2 * me + i] - order_ref[2 * owner + j]) * block
                bias[i * block : (i + 1) * block, j * block : (j + 1) * block] = jnp.where(
                    base + ahead >= 0, 0.0, masked_score
                )

        def one_head(h, inner):
            cols = pl.ds(pl.multiple_of(h * HEAD_DIM, HEAD_DIM), HEAD_DIM)
            keys = ring[step, :, :HEAD_DIM]
            for i in range(2):
                at = pl.ds(i * block, block)
                scores = lax.dot_general(
                    q_ref[at, cols], keys, (((1,), (1,)), ((), ())),
                    preferred_element_type=jnp.float32,
                )
                scores = scores + bias[at, :]
                old_top = top[h, at, :]
                new_top = jnp.maximum(old_top, jnp.max(scores, axis=1, keepdims=True))
                weights = jnp.exp2(scores - new_top).astype(jnp.bfloat16)
                shrink = jnp.exp2(old_top - new_top)
                top[h, at, :] = new_top
                weighted[h, at, :] = weighted[h, at, :] * shrink + jnp.dot(
                    weights, extended[...], preferred_element_type=jnp.float32
                )
            return inner

        lax.fori_loop(0, heads, one_head, 0, unroll=2)
        return carried

    lax.fori_loop(0, n_cp, visit, 0)
    lane = lax.broadcasted_iota(jnp.int32, (rows, HEAD_DIM), 1)
    norms[...] = jnp.zeros_like(norms)
    for h in range(heads):
        totals = weighted[h, :, HEAD_DIM:]
        out_ref[:, h * HEAD_DIM : (h + 1) * HEAD_DIM] = (
            weighted[h, :, :HEAD_DIM] / totals
        ).astype(jnp.bfloat16)
        norm = (top[h] + jnp.log2(totals)) * (1.0 / LOG2E)
        norms[...] = jnp.where(lane == h, norm, norms[...])
    norm_ref[...] = jnp.transpose(norms[...])[:heads, :]

    for step in range(n_cp - 1):
        for h in range(2):
            hop(step, h).wait_send()


def layer_kernel(
    order_hbm, x_hbm, gain_hbm, wq_hbm, wk_hbm, wv_hbm, wo_hbm, turns_hbm, starts_hbm,
    out_ref, norm_ref,
    order_ref, held, weights, out_weights, gains, acc, squares, turns, starts,
    queries, keys, values, weighted, top, from_sib, from_six, from_x, from_y,
    x_sems, w_sems, o_sems, t_sems, relay, ag_send, ag_recv, kv_send, kv_recv, rs_send, rs_recv,
):
    me = lax.axis_index("tp")
    z = lax.axis_index("cp")
    rows, depth = x_hbm.shape
    half = depth // 2
    block = rows // 2
    q_cols = wq_hbm.shape[1]
    k_cols = wk_hbm.shape[1]
    heads = q_cols // HEAD_DIM
    kv_end = q_cols + 2 * k_cols
    sib, nx, ny = flipped(me, 1), flipped(me, 2), flipped(me, 4)
    pieces = ((0, block), (block, block // 2), (block + block // 2, block // 2))

    upper = z // 2
    low = z + upper * (3 - 2 * z)
    others = []
    for k in range(3):
        near = k + 1 - (low if k == 0 else 0)
        others.append(near + upper * (3 - 2 * near))

    x_copies = []
    for p, (first, count) in enumerate(((0, block), (block, block))):
        for h in range(2):
            at = pl.ds(first, count)
            x_copies.append(
                pltpu.make_async_copy(
                    x_hbm.at[at, pl.ds(h * half, half)], held.at[0, h, at, :], x_sems.at[p, h]
                )
            )
    for copy in x_copies:
        copy.start()
    small = [
        pltpu.make_async_copy(gain_hbm, gains, t_sems.at[0]),
        pltpu.make_async_copy(turns_hbm, turns, t_sems.at[1]),
        pltpu.make_async_copy(starts_hbm, starts, t_sems.at[2]),
        pltpu.make_async_copy(order_hbm, order_ref, t_sems.at[3]),
    ]
    small[0].start()
    small[3].start()
    w_copies = []
    for e in range(8):
        chunk = pl.ds(pl.multiple_of(flipped(me, e) * depth, depth), depth)
        parts = ((wq_hbm, 0, q_cols), (wk_hbm, q_cols, k_cols), (wv_hbm, q_cols + k_cols, k_cols))
        w_copies.append(
            [
                pltpu.make_async_copy(
                    w.at[chunk, :], weights.at[e, :, pl.ds(at, size)], w_sems.at[e, i]
                )
                for i, (w, at, size) in enumerate(parts)
            ]
        )
    o_copies = {}
    for e in (7, 6, 3, 2, 5, 4, 1, 0):
        for h in range(2):
            at = pl.ds(pl.multiple_of(flipped(me, e) * depth + h * half, half), half)
            o_copies[e, h] = pltpu.make_async_copy(
                wo_hbm.at[:, at], out_weights.at[e, h], o_sems.at[e, h]
            )

    barrier = pltpu.get_barrier_semaphore()
    inner = (z + 1) // 2 % 2

    def tell(semaphore, device):
        pl.semaphore_signal(semaphore, inc=1, device_id=device, device_id_type=MESH)

    for other in (sib, nx, ny):
        tell(barrier, {"tp": other})
    tell(barrier, {"cp": others[0]})

    @pl.when(inner == 1)
    def _():
        tell(barrier, {"cp": 3 - z})

    pl.semaphore_wait(barrier, 4 + inner)

    @pl.when(inner == 1)
    def _():
        tell(relay, {"cp": 3 - z})

    def remote(source, target, send, recv, device):
        return pltpu.make_async_remote_copy(
            src_ref=source, dst_ref=target, send_sem=send, recv_sem=recv,
            device_id=device, device_id_type=MESH,
        )

    gather = []
    for p, (first, count) in enumerate(pieces):
        at = pl.ds(first, count)

        def part(slot, h, at=at):
            return held.at[slot, h, at, :]

        plan = {
            "dx0": (0, 0, 2, nx), "dx1": (0, 1, 2, nx), "dy0": (0, 0, 4, ny), "dy1": (0, 1, 4, ny),
            "s0": (0, 0, 1, sib), "s1": (0, 1, 1, sib), "fy": (2, 0, 6, ny), "fx": (4, 1, 6, nx),
            "a0": (2, 0, 3, sib), "a1": (2, 1, 3, sib), "b0": (4, 0, 5, sib), "b1": (4, 1, 5, sib),
            "c0": (6, 0, 7, sib), "c1": (6, 1, 7, sib),
        }
        gather.append(
            {
                name: remote(
                    part(slot, h), part(to, h), ag_send.at[p, i], ag_recv.at[p, i], {"tp": other}
                )
                for i, (name, (slot, h, to, other)) in enumerate(plan.items())
            }
        )

    def send(p, *names):
        for name in names:
            gather[p][name].start()

    def landed(p, *names):
        for name in names:
            gather[p][name].wait_recv()

    for copy in x_copies[:2]:
        copy.wait()
    send(0, "dx0", "dy1", "dx1", "dy0", "s0", "s1")
    for copies in w_copies:
        for copy in copies:
            copy.start()
    small[1].start()
    small[2].start()
    acc[...] = jnp.zeros_like(acc)
    squares[...] = jnp.zeros_like(squares)
    values[:, HEAD_DIM:, :] = jnp.ones((4, 16, rows), jnp.bfloat16)
    for copy in x_copies[2:]:
        copy.wait()
    for p in (1, 2):
        send(p, "s0", "s1")
    small[0].wait()

    def weights_of(*slots):
        for e in slots:
            for copy in w_copies[e]:
                copy.wait()

    def process(first, count, chunks, chunk_of, low=0, high=kv_end):
        at = pl.ds(first, count)

        @pl.loop(0, chunks // 2)
        def _(i):
            total = None
            for u in range(2):
                e, h = chunk_of(2 * i + u)
                wide = held[e, h, at, :].astype(jnp.float32)
                if high == kv_end:
                    squares[at, :] += jnp.sum(wide * wide, axis=1, keepdims=True)
                piece = jnp.dot(
                    (wide * gains[flipped(me, e), h]).astype(jnp.bfloat16),
                    weights[e, pl.ds(pl.multiple_of(h * half, half), half), low:high],
                    preferred_element_type=jnp.float32,
                )
                total = piece if total is None else total + piece
            acc[at, low:high] += total

    def own_pair(i):
        return i // 2, i % 2

    def early(i):
        return 2 + i, i // 2

    def late(i):
        return 2 + i, 1 - i // 2

    def last_two(i):
        return 6 + i // 2, i % 2

    score_scale = LOG2E / math.sqrt(HEAD_DIM)
    features = depth * 8

    def exchange(p, k, which):
        first, count = pieces[p]
        if which == 0:
            ref = keys.at[z, pl.ds(first, count), :]
        else:
            ref = values.at[z, pl.ds(0, HEAD_DIM), pl.ds(first, count)]
        return remote(ref, ref, kv_send.at[p, k, which], kv_recv.at[p, z, which], {"cp": others[k]})

    def arrived(p, owner):
        first, count = pieces[p]
        refs = (
            keys.at[owner, pl.ds(first, count), :],
            values.at[owner, pl.ds(0, HEAD_DIM), pl.ds(first, count)],
        )
        for which, ref in enumerate(refs):
            remote(
                ref, ref, kv_send.at[p, 0, which], kv_recv.at[p, owner, which], {"cp": others[0]}
            ).wait_recv()

    def turner(first, j, sub):
        start = starts[order_ref[2 * z + first // block]]
        at = pl.ds(pl.multiple_of(first % block + j * sub, sub), sub)
        cosine = turns[0, at, :] * start[0:1, :] - turns[1, at, :] * start[1:2, :]
        sine = turns[1, at, :] * start[2:3, :] + turns[0, at, :] * start[3:4, :]
        even = lax.rem(lax.broadcasted_iota(jnp.int32, (sub, HEAD_DIM), 1), 2) == 0

        def turned(content):
            later = pltpu.roll(content, HEAD_DIM - 1, 1)
            former = pltpu.roll(content, 1, 1)
            return content * cosine + jnp.where(even, later, former) * sine

        return turned

    def rate_of(at):
        return lax.rsqrt(squares[at, :] * (1.0 / features) + norm_epsilon)

    def finish_keys(p):
        first, count = pieces[p]

        @pl.loop(0, count // 128)
        def _(j):
            at = pl.ds(pl.multiple_of(first + j * 128, 128), 128)
            rate = rate_of(at)
            turned = turner(first, j, 128)
            keys[z, at, :] = turned(acc[at, q_cols : q_cols + k_cols] * rate).astype(jnp.bfloat16)
            value = acc[at, q_cols + k_cols : kv_end] * rate
            values[z, :HEAD_DIM, at] = jnp.transpose(value).astype(jnp.bfloat16)

        for k in (0, 2, 1):
            for which in (0, 1):
                exchange(p, k, which).start()

    def finish_queries(p):
        first, count = pieces[p]

        @pl.loop(0, count // 64)
        def _(j):
            at = pl.ds(pl.multiple_of(first + j * 64, 64), 64)
            rate = rate_of(at) * score_scale
            turned = turner(first, j, 64)
            for h in range(heads):
                cols = pl.ds(h * HEAD_DIM, HEAD_DIM)
                queries[at, cols] = turned(acc[at, cols] * rate).astype(jnp.bfloat16)

    def visible(s, owner, j):
        ahead = order_ref[2 * z + s] - order_ref[2 * owner + j]
        return jnp.where(ahead > 0, 0.0, masked_score)

    def attend(s, chunks, together, start=False, finish=False):
        q_at = pl.ds(s * block, block)
        shades = {}
        for chunk in chunks:
            for owner, first, count, diagonal in chunk:
                if not diagonal:
                    shades[id(owner), first] = visible(s, owner, first // block)

        def columns(h):
            return pl.ds(pl.multiple_of(h * HEAD_DIM, HEAD_DIM), HEAD_DIM)

        def place(side, j, offset, count):
            return pl.ds(side * block + offset, count), pl.ds(j * block, block)

        def scored(h, side, j, peak):
            offset = 0
            for owner, first, count, diagonal in chunks[j]:
                scores = lax.dot_general(
                    keys[owner, pl.ds(first, count), :], queries[q_at, columns(h)],
                    (((1,), (1,)), ((), ())), preferred_element_type=jnp.float32,
                )
                if diagonal:
                    key_at = lax.broadcasted_iota(jnp.int32, (count, block), 0)
                    query_at = lax.broadcasted_iota(jnp.int32, (count, block), 1)
                    scores = jnp.where(key_at <= query_at, scores, masked_score)
                acc[place(side, j, offset, count)] = scores
                offset += count
                highest = jnp.max(scores, axis=0, keepdims=True)
                if not diagonal:
                    highest = highest + shades[id(owner), first]
                peak = highest if peak is None else jnp.maximum(peak, highest)
            return peak

        def beside(coming, side, h, peak):
            slot = s * heads + h
            new_top = peak
            if not start:
                old_top = top[slot]
                new_top = jnp.maximum(old_top, peak)
                shrink = jnp.exp2(old_top - new_top)
            next_peak, total = None, None
            for j, chunk in enumerate(chunks):
                if coming is not None:
                    next_peak = scored(coming, 1 - side, j, next_peak)
                offset = 0
                shares, extended = [], []
                for owner, first, count, diagonal in chunk:
                    lean = new_top if diagonal else new_top - shades[id(owner), first]
                    scores = acc[place(side, j, offset, count)]
                    shares.append(jnp.exp2(scores - lean).astype(jnp.bfloat16))
                    extended.append(values[owner, :, pl.ds(first, count)])
                    offset += count
                share, wide = shares[0], extended[0]
                if len(chunk) > 1:
                    share, wide = jnp.concatenate(shares, 0), jnp.concatenate(extended, 1)
                piece = jnp.dot(wide, share, preferred_element_type=jnp.float32)
                total = piece if total is None else total + piece
            if not start:
                total = weighted[slot] * shrink + total
            if finish:
                sums = total[HEAD_DIM : HEAD_DIM + 1, :]
                part = total[:HEAD_DIM, :] * (1.0 / sums)
                queries[q_at, columns(h)] = jnp.transpose(part).astype(jnp.bfloat16)
                norm_ref[pl.ds(h, 1), q_at] = (new_top + jnp.log2(sums)) * (1.0 / LOG2E)
            else:
                weighted[slot] = total
                top[slot] = new_top
            return next_peak

        peak = None
        for j in range(len(chunks)):
            peak = scored(0, 0, j, peak)
        if together == heads:
            for h in range(heads):
                peak = beside(h + 1 if h + 1 < heads else None, h % 2, h, peak)
        else:

            def group(i, peak):
                for u in range(together):
                    h = i * together + u
                    coming = h + 1 if u + 1 < together else jnp.minimum(h + 1, heads - 1)
                    peak = beside(coming, u % 2, h, peak)
                return peak

            lax.fori_loop(0, heads // together, group, peak)

    weights_of(0, 1)
    landed(0, "s0", "s1")
    process(*pieces[0], 4, own_pair)

    @pl.when(inner == 1)
    def _():
        pl.semaphore_wait(relay, 1)
        tell(relay, {"cp": others[0]})

    landed(0, "dx0")
    send(0, "fy", "a0")
    landed(0, "dy1")
    send(0, "fx", "b1")
    send(1, "dx0", "dy1", "dx1", "dy0")
    send(2, "dx0", "dy1")
    for copy in o_copies.values():
        copy.start()
    weights_of(2, 3, 4, 5)
    landed(0, "a0", "b1")
    process(*pieces[0], 4, early)
    landed(0, "dx1")
    send(0, "a1")
    landed(0, "dy0")
    send(0, "b0")
    for p in (1, 2):
        landed(p, "s0", "s1")
    process(block, block, 4, own_pair)
    landed(0, "a1", "b0")
    process(*pieces[0], 4, late)
    weights_of(6, 7)
    landed(0, "fy")
    send(0, "c0")
    landed(0, "fx")
    send(0, "c1")
    process(*pieces[0], 2, lambda i: (6, i), q_cols)
    for copy in small[1:]:
        copy.wait()

    @pl.when(inner == 0)
    def _():
        pl.semaphore_wait(relay, 1)

    landed(0, "c0", "c1")
    process(*pieces[0], 2, lambda i: (7, i), q_cols)
    finish_keys(0)
    landed(1, "dx0")
    send(1, "fy", "a0")
    landed(1, "dy1")
    send(1, "fx", "b1")
    send(2, "dx1", "dy0")
    process(*pieces[0], 4, last_two, 0, q_cols)
    finish_queries(0)
    landed(1, "a0", "b1")
    process(*pieces[1], 4, early)
    landed(1, "dx1")
    send(1, "a1")
    landed(1, "dy0")
    send(1, "b0")
    landed(1, "a1", "b0")
    process(*pieces[1], 4, late)
    landed(2, "dx0")
    send(2, "fy", "a0")
    landed(2, "dy1")
    send(2, "fx", "b1")
    landed(2, "a0", "b1")
    process(*pieces[2], 4, early)
    landed(1, "fy")
    send(1, "c0")
    landed(1, "fx")
    send(1, "c1")
    process(*pieces[1], 2, lambda i: (6, i), q_cols)
    landed(1, "c0", "c1")
    process(*pieces[1], 2, lambda i: (7, i), q_cols)
    finish_keys(1)
    process(*pieces[1], 4, last_two, 0, q_cols)
    finish_queries(1)
    third = block // 2
    near, middle, distant = others
    landed(2, "dx1")
    send(2, "a1")
    landed(2, "dy0")
    send(2, "b0")
    landed(2, "a1", "b0")
    process(*pieces[2], 4, late)
    landed(2, "fy")
    send(2, "c0")
    landed(2, "fx")
    send(2, "c1")
    process(*pieces[2], 2, lambda i: (6, i), q_cols)
    landed(2, "c0", "c1")
    process(*pieces[2], 2, lambda i: (7, i), q_cols)
    finish_keys(2)
    process(*pieces[2], 4, last_two, 0, q_cols)
    finish_queries(2)

    for owner in others:
        arrived(0, owner)
    whole = [[(owner, 0, block, False)] for owner in others]
    attend(0, [[(z, 0, block, True)], [(z, block, block, False)]] + whole, 4, start=True)
    for owner in others:
        arrived(1, owner)
    attend(
        0,
        [
            [(near, block, third, False), (middle, block, third, False)],
            [(distant, block, third, False)],
        ],
        4,
    )
    for p in range(3):
        for copy in gather[p].values():
            copy.wait_send()
    for owner in others:
        arrived(2, owner)
    attend(
        0,
        [
            [(near, block + third, third, False), (middle, block + third, third, False)],
            [(distant, block + third, third, False)],
        ],
        heads,
        finish=True,
    )

    scatter = []
    for s in range(2):
        at = pl.ds(s * block, block)
        plan = {}
        for e in (1, 3, 5, 7):
            for h in range(2):
                plan["s", e, h] = (held.at[e, h, at, :], from_sib.at[e // 2, h, at, :], sib)
        plan["six", 0] = (held.at[6, 0, at, :], from_six.at[0, at, :], nx)
        plan["six", 1] = (held.at[6, 1, at, :], from_six.at[1, at, :], ny)
        for h in range(2):
            plan["x", h] = (held.at[2, h, at, :], from_x.at[h, at, :], nx)
            plan["y", h] = (held.at[4, h, at, :], from_y.at[h, at, :], ny)
        scatter.append(
            {
                name: remote(source, target, rs_send.at[s, i], rs_recv.at[s, i], {"tp": other})
                for i, (name, (source, target, other)) in enumerate(plan.items())
            }
        )

    def term(s, e, h):
        if s == 0:
            o_copies[e, h].wait()
        at = pl.ds(s * block, block)
        held[e, h, at, :] = jnp.dot(
            queries[at, :], out_weights[e, h], preferred_element_type=jnp.float32
        ).astype(jnp.bfloat16)
        if e % 2:
            scatter[s]["s", e, h].start()

    def summed(s, e, h, more=()):
        scatter[s]["s", e + 1, h].wait_recv()

        @pl.loop(0, block // 64)
        def _(i):
            at = pl.ds(pl.multiple_of(s * block + i * 64, 64), 64)
            total = held[e, h, at, :].astype(jnp.float32)
            total = total + from_sib[e // 2, h, at, :].astype(jnp.float32)
            for other in more:
                total = total + other[at, :].astype(jnp.float32)
            if e:
                held[e, h, at, :] = total.astype(jnp.bfloat16)
            else:
                out_ref[at, h * half : (h + 1) * half] = total.astype(jnp.bfloat16)

    def far(s):
        term(s, 7, 0)
        term(s, 7, 1)
        term(s, 6, 0)
        summed(s, 6, 0)
        scatter[s]["six", 0].start()
        term(s, 6, 1)
        summed(s, 6, 1)
        scatter[s]["six", 1].start()
        term(s, 3, 0)
        term(s, 5, 1)
        term(s, 2, 0)
        summed(s, 2, 0)
        scatter[s]["x", 0].start()
        term(s, 4, 1)
        summed(s, 4, 1)
        scatter[s]["y", 1].start()
        term(s, 3, 1)

    def near(s):
        term(s, 2, 1)
        term(s, 5, 0)
        term(s, 4, 0)
        scatter[s]["six", 0].wait_recv()
        summed(s, 4, 0, (from_six.at[0],))
        scatter[s]["y", 0].start()
        scatter[s]["six", 1].wait_recv()
        summed(s, 2, 1, (from_six.at[1],))
        scatter[s]["x", 1].start()

    def last(s):
        for h in range(2):
            scatter[s]["x", h].wait_recv()
            scatter[s]["y", h].wait_recv()
            summed(s, 0, h, (from_x.at[h], from_y.at[h]))

    far(0)
    attend(1, [[(z, block, block, True)], [(z, 0, block, False)]] + whole, 4, start=True)
    near(0)
    attend(1, [[(owner, block, block, False)] for owner in others], 4, finish=True)
    far(1)
    for s in range(2):
        for h in range(2):
            term(s, 1, h)
            term(s, 0, h)
    near(1)
    last(0)
    last(1)
    for p in range(3):
        for k in range(3):
            for which in range(2):
                exchange(p, k, which).wait_send()
    for s in range(2):
        for copy in scatter[s].values():
            copy.wait_send()


def rotary_tables(block, count):
    lanes = np.arange(HEAD_DIM)
    rates = rope_base ** (-2.0 * (lanes // 2) / HEAD_DIM)
    sign = np.where(lanes % 2 == 0, -1.0, 1.0)
    inside = np.arange(block)[:, None] * rates[None, :]
    turns = np.stack([np.cos(inside), np.sin(inside)]).astype(np.float32)
    begin = (np.arange(count) * block)[:, None] * rates[None, :]
    cosine, sine = np.cos(begin), np.sin(begin)
    starts = np.stack([cosine, sine, sign * cosine, sign * sine], axis=1)
    starts = np.concatenate([starts, np.zeros_like(starts)], axis=1).astype(np.float32)
    return jnp.asarray(turns), jnp.asarray(starts)


def store_kernel(out_ref, norm_ref, out_hbm, norm_hbm, sems):
    copies = [
        pltpu.make_async_copy(out_ref, out_hbm, sems.at[0]),
        pltpu.make_async_copy(norm_ref, norm_hbm, sems.at[1]),
    ]
    for copy in copies:
        copy.start()
    for copy in copies:
        copy.wait()


def fused_shards(
    n_cp, n_tp, checkpoint, norm_gain, query_weight, key_weight, value_weight, output_weight, block_order
):
    rows, depth = checkpoint.shape
    q_cols = query_weight.shape[1]
    k_cols = key_weight.shape[1]
    heads = q_cols // HEAD_DIM
    block = rows // 2
    half = depth // 2
    bf16, f32 = jnp.bfloat16, jnp.float32
    turns, starts = rotary_tables(block, block_order.shape[0])
    any_spec = pl.BlockSpec(memory_space=pl.ANY)
    vmem = pl.BlockSpec(memory_space=pltpu.VMEM)
    dma = pltpu.SemaphoreType.DMA
    results = pl.pallas_call(
        layer_kernel,
        out_shape=(pltpu.VMEM((rows, depth), bf16), pltpu.VMEM((heads, rows), f32)),
        in_specs=[any_spec] * 9,
        out_specs=(vmem, vmem),
        scratch_shapes=[
            pltpu.SMEM(block_order.shape, jnp.int32),
            pltpu.VMEM((8, 2, rows, half), bf16),
            pltpu.VMEM((8, depth, q_cols + 2 * k_cols), bf16),
            pltpu.VMEM((8, 2, q_cols, half), bf16),
            pltpu.VMEM((8, 2, 1, half), f32),
            pltpu.VMEM((rows, q_cols + 2 * k_cols), f32),
            pltpu.VMEM((rows, 1), f32),
            pltpu.VMEM((2, block, HEAD_DIM), f32),
            pltpu.VMEM(starts.shape, f32),
            pltpu.VMEM((rows, q_cols), bf16),
            pltpu.VMEM((n_cp, rows, HEAD_DIM), bf16),
            pltpu.VMEM((n_cp, HEAD_DIM + 16, rows), bf16),
            pltpu.VMEM((2 * heads, HEAD_DIM + 16, block), f32),
            pltpu.VMEM((2 * heads, 1, block), f32),
            pltpu.VMEM((4, 2, rows, half), bf16),
            pltpu.VMEM((2, rows, half), bf16),
            pltpu.VMEM((2, rows, half), bf16),
            pltpu.VMEM((2, rows, half), bf16),
            dma((2, 2)),
            dma((8, 3)),
            dma((8, 2)),
            dma((4,)),
            pltpu.SemaphoreType.REGULAR,
            dma((3, 14)),
            dma((3, 14)),
            dma((3, n_cp - 1, 2)),
            dma((3, n_cp, 2)),
            dma((2, 14)),
            dma((2, 14)),
        ],
        compiler_params=pltpu.CompilerParams(
            collective_id=0, has_side_effects=True, vmem_limit_bytes=FUSED_BYTES
        ),
        name="layer",
    )(
        block_order, checkpoint, norm_gain.reshape(8, 2, 1, half), query_weight, key_weight,
        value_weight, output_weight, turns, starts,
    )
    return pl.pallas_call(
        store_kernel,
        out_shape=(
            jax.ShapeDtypeStruct((rows, depth), bf16),
            jax.ShapeDtypeStruct((heads, rows), f32),
        ),
        in_specs=[vmem, vmem],
        out_specs=(any_spec, any_spec),
        scratch_shapes=[dma((2,))],
        compiler_params=pltpu.CompilerParams(vmem_limit_bytes=1 << 20),
        name="store",
    )(*results)


def shards(
    n_cp, n_tp, checkpoint, norm_gain, query_weight, key_weight, value_weight, output_weight, block_order
):
    rows = checkpoint.shape[0]
    q_cols = query_weight.shape[1]
    heads = q_cols // HEAD_DIM
    block = rows // 2
    context_rank = lax.axis_index("cp")
    own_blocks = lax.dynamic_slice_in_dim(block_order, 2 * context_rank, 2)
    offsets = jnp.arange(block, dtype=jnp.int32)
    positions = (own_blocks[:, None] * block + offsets[None, :]).reshape(rows)

    vmem = pl.BlockSpec(memory_space=pltpu.VMEM)
    smem = pl.BlockSpec(memory_space=pltpu.SMEM)
    bf16, f32 = jnp.bfloat16, jnp.float32
    dma = pltpu.SemaphoreType.DMA
    queries, key_value = project_any(
        checkpoint, norm_gain, query_weight, key_weight, value_weight, positions
    )
    attended, normalizer = pl.pallas_call(
        functools.partial(attend_kernel, n_cp),
        out_shape=(
            jax.ShapeDtypeStruct((rows, q_cols), bf16),
            jax.ShapeDtypeStruct((heads, rows), f32),
        ),
        in_specs=[smem, vmem, pl.BlockSpec(memory_space=pl.ANY)],
        out_specs=(vmem, vmem),
        scratch_shapes=[
            pltpu.VMEM((n_cp, rows, 2 * HEAD_DIM), bf16),
            pltpu.VMEM((rows, 2 * HEAD_DIM), bf16),
            pltpu.VMEM((rows, rows), f32),
            pltpu.VMEM((heads, rows, 1), f32),
            pltpu.VMEM((heads, rows, 2 * HEAD_DIM), f32),
            pltpu.VMEM((rows, HEAD_DIM), f32),
            dma,
            dma((n_cp - 1, 2)),
            dma((n_cp - 1, 2)),
        ],
        compiler_params=pltpu.CompilerParams(
            collective_id=1, has_side_effects=True, vmem_limit_bytes=VMEM_BYTES
        ),
        name="attend",
    )(block_order, queries, key_value)
    partial_terms = jnp.dot(attended, output_weight, preferred_element_type=jnp.float32)
    projected = lax.psum_scatter(partial_terms.astype(bf16), "tp", scatter_dimension=1, tiled=True)
    return (projected, normalizer)


def solution(mesh):
    n_cp, n_tp = mesh.shape["cp"], mesh.shape["tp"]
    body = fused_shards if (n_cp, n_tp) == (4, 8) else shards
    return jax.shard_map(
        functools.partial(body, n_cp, n_tp),
        mesh=mesh,
        in_specs=(
            P("cp", "tp"),
            P(),
            P(None, "tp"),
            P(None, "tp"),
            P(None, "tp"),
            P("tp", None),
            P(),
        ),
        out_specs=(P("cp", "tp"), P("tp", "cp")),
        check_vma=False,
    )
```
